32 devices in a mesh: fsdp: 4 (over y, x), tp: 8 (over z, core).
Axes of the slice: x: 2, y: 2, z: 4, core: 2. Of those that a mesh axis runs over, the one named last changes fastest.
Arguments:
- ref_gate: bfloat16 [3072, 11008], P('fsdp', 'tp'), may hold values from -6 to 6
- ref_up: bfloat16 [3072, 11008], P('fsdp', 'tp'), may hold values from -6 to 6
- ref_residual: bfloat16 [3072, 4096], P('fsdp', 'tp'), may hold values from -6 to 6
- ref_modality: int32 [3072], P('fsdp'), may hold values 0 or 1
- ref_down_text: bfloat16 [4096, 11008], P('fsdp', 'tp'), may hold values from -0.0546875 to 0.0546875
- ref_down_image: bfloat16 [4096, 11008], P('fsdp', 'tp'), may hold values from -0.0546875 to 0.0546875
- pol_gate: bfloat16 [3072, 11008], P('fsdp', 'tp'), may hold values from -6 to 6
- pol_up: bfloat16 [3072, 11008], P('fsdp', 'tp'), may hold values from -6 to 6
- pol_modality: int32 [3072], P('fsdp'), may hold values 0 or 1
- pol_segment: int32 [3072], P('fsdp'), may hold values from 0 to 5, never falling along the last dimension, each value on 1 to 768 neighbouring positions
- pair_margin: float32 [3], replicated, may hold values from -30 to 30
- token_cotangent: bfloat16 [3072, 4096], P('fsdp', 'tp'), may hold values from -24 to 24
- pol_down_text: bfloat16 [4096, 11008], P('fsdp', 'tp'), may hold values from -0.0546875 to 0.0546875
- pol_down_image: bfloat16 [4096, 11008], P('fsdp', 'tp'), may hold values from -0.0546875 to 0.0546875
Outputs:
- ref_out: bfloat16 [3072, 4096], P('fsdp', 'tp')
- grad_gate: bfloat16 [3072, 11008], P('fsdp', 'tp')
- grad_up: bfloat16 [3072, 11008], P('fsdp', 'tp')
- grad_down_text: float32 [4096, 11008], P('fsdp', 'tp')
- grad_down_image: float32 [4096, 11008], P('fsdp', 'tp')
The draws below stay inside these ranges and needn't reach their ends.
Inputs may be any that keep to these rules, and one draw needn't show every extreme that they name: `ref_modality`: 0 marks a text token, 1 an image token. `pol_modality`: 0 marks a text token, 1 an image token. `pol_segment`: response numbers never fall along the tokens; responses 2p and 2p + 1 are the chosen and the rejected response of pair p; every response has at least one token.
All inputs are finite; a program needn't handle non-finite values. No bound on the sum of `ref_modality` or of `pol_modality` on one device may be relied on, other than what follows from the above.
Results may differ from the reference program's by a relative error of at most 0.015.
Values may be sent and summed in bfloat16 or wider, within the bound.
A program may use at most 192 MiB of HBM per device.

```python
import math
import jax
import jax.numpy as jnp
import numpy as np
from jax import lax

D = 4096
FF = 11008
SEQ = 512
TOKENS = 3072
PAIRS = 3
N_FSDP = 4
N_TP = 8


def plant(entries, rng, smallest, top_value):
    longest = entries.shape.index(max(entries.shape))
    spots = []
    for shift in (0, 1):
        where = [jax.random.randint(jax.random.fold_in(rng, axis), (), 0, length) for axis, length in enumerate(entries.shape)]
        where[longest] = (where[longest] + shift) % entries.shape[longest]
        spots.append(tuple(where))
    return entries.at[spots[0]].set(smallest).at[spots[1]].set(top_value)


def block_levels(own_key, dims, pieces, least, largest):
    def one(position, shards_of):
        steps = jax.random.uniform(jax.random.fold_in(jax.random.fold_in(own_key, 6), position), (shards_of,), jnp.float32, least / len(pieces), largest / len(pieces))
        return jnp.repeat(jnp.exp(steps), dims[position] // shards_of).reshape((-1,) + (1,) * (len(dims) - position - 1))

    factor_of = one(*pieces[0])
    for cut in pieces[1:]:
        factor_of = factor_of * one(*cut)
    return factor_of


def profile(number_of, total, bound, slope):
    weights = [(1 << 20) // math.isqrt(standing ** slope) + 1 for standing in range(2, number_of + 1)]
    spare, counts = total - bound - (number_of - 1), [1] * (number_of - 1)
    while spare > 0:
        movable = [i for i in range(number_of - 1) if counts[i] < bound]
        whole, left = sum([weights[i] for i in movable]), spare
        for i in movable:
            extra = min(bound - counts[i], max(1, left * weights[i] // whole), spare)
            counts[i] = counts[i] + extra
            spare = spare - extra
    return np.array([bound] + counts)


def ragged_sizes(own_key, amount, total, bound, lean):
    if amount == 2:
        one = jax.random.randint(own_key, (), max(1, total - bound), min(bound, total - 1) + 1)
        return jnp.stack([one, total - one])
    lengths = jnp.asarray(profile(amount, total, bound, lean), jnp.int32)
    twos = (amount - 1) // 2
    source_of, receiver = lengths[1:1 + 2 * twos:2], lengths[2:2 + 2 * twos:2]
    margin = jnp.minimum(source_of - 1, bound - receiver)
    shifted = jax.random.randint(jax.random.fold_in(own_key, 1), (twos,), 0, 1 << 20) % (margin + 1)
    lengths = lengths.at[1:1 + 2 * twos:2].set(source_of - shifted).at[2:2 + 2 * twos:2].set(receiver + shifted)
    return lengths[jax.random.permutation(jax.random.fold_in(own_key, 2), amount)]


def normal_values(rng, dims, deviation, limit, pieces=(), held_as=jnp.bfloat16):
    factor_of = block_levels(rng, dims, pieces, -0.22, 0.18) if pieces else 1.0
    result = jax.random.normal(rng, dims, jnp.float32) * deviation * factor_of
    return jnp.minimum(jnp.maximum(result, -limit), limit).astype(held_as)


def setup_inputs(seed: int = 0) -> dict:
    seeds = jax.random.split(jax.random.key(seed), 15)
    ref_gate = normal_values(seeds[0], (TOKENS, FF), 1.0, 6.0, ((0, 4), (1, 8)))
    ref_up = normal_values(seeds[1], (TOKENS, FF), 1.0, 6.0, ((0, 4), (1, 8)))
    ref_residual = normal_values(seeds[2], (TOKENS, D), 1.0, 6.0, ((0, 4), (1, 8)))
    ref_modality = plant((jax.random.randint(seeds[3], (TOKENS,), 0, 5) < 2).astype(jnp.int32), jax.random.fold_in(seeds[3], 1), 0, 1)
    ref_down_text = normal_values(seeds[4], (D, FF), FF ** -0.5, 0.0546875, ((0, 4), (1, 8)))
    ref_down_image = normal_values(seeds[5], (D, FF), FF ** -0.5, 0.0546875, ((0, 4), (1, 8)))
    pol_gate = normal_values(seeds[6], (TOKENS, FF), 1.0, 6.0, ((0, 4), (1, 8)))
    pol_up = normal_values(seeds[7], (TOKENS, FF), 1.0, 6.0, ((0, 4), (1, 8)))
    pol_modality = plant((jax.random.randint(seeds[8], (TOKENS,), 0, 5) < 2).astype(jnp.int32), jax.random.fold_in(seeds[8], 1), 0, 1)
    pol_segment = jnp.searchsorted(jnp.cumsum(ragged_sizes(seeds[9], 2 * PAIRS, TOKENS, SEQ + SEQ // 2, 0)), jnp.arange(TOKENS), side="right").astype(jnp.int32)
    pair_margin = jnp.clip(jax.random.uniform(seeds[10], (PAIRS,), jnp.float32, -30.0, 30.0), -30.0, 30.0)
    token_cotangent = normal_values(seeds[11], (TOKENS, D), 4.0, 24.0, ((0, 4), (1, 8)))
    pol_down_text = normal_values(seeds[12], (D, FF), FF ** -0.5, 0.0546875, ((0, 4), (1, 8)))
    pol_down_image = normal_values(seeds[13], (D, FF), FF ** -0.5, 0.0546875, ((0, 4), (1, 8)))
    return {"ref_gate": ref_gate, "ref_up": ref_up, "ref_residual": ref_residual, "ref_modality": ref_modality, "ref_down_text": ref_down_text, "ref_down_image": ref_down_image, "pol_gate": pol_gate, "pol_up": pol_up, "pol_modality": pol_modality, "pol_segment": pol_segment, "pair_margin": pair_margin, "token_cotangent": token_cotangent, "pol_down_text": pol_down_text, "pol_down_image": pol_down_image}


dpo_beta = 0.1


def split_hidden(gate, up, modality):
    gate_f = gate.astype(jnp.float32)
    up_f = up.astype(jnp.float32)
    sig = jax.nn.sigmoid(gate_f)
    act = gate_f * sig
    hidden = (act * up_f).astype(jnp.bfloat16)
    image = (modality == 1)[:, None]
    zero = jnp.zeros_like(hidden)
    return jnp.where(image, zero, hidden), jnp.where(image, hidden, zero), gate_f, up_f, sig, act


def reference(ref_gate, ref_up, ref_residual, ref_modality, ref_down_text, ref_down_image, pol_gate, pol_up, pol_modality, pol_segment, pair_margin, token_cotangent, pol_down_text, pol_down_image):
    ref_text, ref_image, _, _, _, _ = split_hidden(ref_gate, ref_up, ref_modality)
    block_width = FF // N_TP
    contract = (((1,), (1,)), ((), ()))

    def ref_block(index, total):
        start = (index * block_width).astype(jnp.int32)
        left_text = lax.dynamic_slice_in_dim(ref_text, start, block_width, 1)
        left_image = lax.dynamic_slice_in_dim(ref_image, start, block_width, 1)
        right_text = lax.dynamic_slice_in_dim(ref_down_text, start, block_width, 1)
        right_image = lax.dynamic_slice_in_dim(ref_down_image, start, block_width, 1)
        part = lax.dot_general(left_text, right_text, contract, preferred_element_type=jnp.float32)
        part = part + lax.dot_general(left_image, right_image, contract, preferred_element_type=jnp.float32)
        rounded = lax.optimization_barrier(part.astype(jnp.bfloat16))
        return total + rounded.astype(jnp.float32)

    summed = lax.fori_loop(0, N_TP, ref_block, jnp.zeros((TOKENS, D), jnp.float32))
    ref_out = (summed + ref_residual.astype(jnp.float32)).astype(jnp.bfloat16)

    pol_text, pol_image, gate_f, up_f, sig, act = split_hidden(pol_gate, pol_up, pol_modality)
    seg_ids = jnp.arange(2 * PAIRS, dtype=jnp.int32)
    pair_weight = dpo_beta * jax.nn.sigmoid(-dpo_beta * pair_margin)
    table = jnp.repeat(pair_weight, 2) * jnp.where(seg_ids % 2 == 0, -1.0, 1.0).astype(jnp.float32)
    coef = jnp.sum(jnp.where(pol_segment[:, None] == seg_ids[None, :], table[None, :], jnp.float32(0.0)), axis=1)
    cot = (coef[:, None] * token_cotangent.astype(jnp.float32)).astype(jnp.bfloat16)
    image_p = (pol_modality == 1)[:, None]
    zero_cot = jnp.zeros_like(cot)
    cot_text = jnp.where(image_p, zero_cot, cot)
    cot_image = jnp.where(image_p, cot, zero_cot)
    d_hidden = jnp.dot(cot_text, pol_down_text, preferred_element_type=jnp.float32)
    d_hidden = d_hidden + jnp.dot(cot_image, pol_down_image, preferred_element_type=jnp.float32)
    grad_gate = (d_hidden * up_f * sig * (1.0 + gate_f * (1.0 - sig))).astype(jnp.bfloat16)
    grad_up = (d_hidden * act).astype(jnp.bfloat16)

    rows_block = TOKENS // N_FSDP
    over_rows = (((0,), (0,)), ((), ()))

    def grad_block(index, totals):
        start = (index * rows_block).astype(jnp.int32)
        y_text = lax.dynamic_slice_in_dim(cot_text, start, rows_block, 0)
        y_image = lax.dynamic_slice_in_dim(cot_image, start, rows_block, 0)
        h_text = lax.dynamic_slice_in_dim(pol_text, start, rows_block, 0)
        h_image = lax.dynamic_slice_in_dim(pol_image, start, rows_block, 0)
        term_text = lax.dot_general(y_text, h_text, over_rows, preferred_element_type=jnp.float32)
        term_image = lax.dot_general(y_image, h_image, over_rows, preferred_element_type=jnp.float32)
        term_text = lax.optimization_barrier(term_text.astype(jnp.bfloat16)).astype(jnp.float32)
        term_image = lax.optimization_barrier(term_image.astype(jnp.bfloat16)).astype(jnp.float32)
        return (totals[0] + term_text, totals[1] + term_image)

    start_grads = (jnp.zeros((D, FF), jnp.float32), jnp.zeros((D, FF), jnp.float32))
    grad_down_text, grad_down_image = lax.fori_loop(0, N_FSDP, grad_block, start_grads)
    return (ref_out, grad_gate, grad_up, grad_down_text, grad_down_image)
```

```python
import jax
import jax.numpy as jnp
from jax import lax
from jax.experimental import pallas as pl
from jax.experimental.pallas import tpu as pltpu
from jax.sharding import PartitionSpec as P


MESH = pl.DeviceIdType.MESH
LANES = 128
VMEM_BYTES = 67043328

dpo_beta = 0.1


def silu_parts(gate, up):
    gate_f = gate.astype(jnp.float32)
    up_f = up.astype(jnp.float32)
    sig = jax.nn.sigmoid(gate_f)
    act = gate_f * sig
    return gate_f, up_f, sig, act


def hidden_of(gate, up):
    _, up_f, _, act = silu_parts(gate, up)
    return (act * up_f).astype(jnp.bfloat16)


def coef_of(pol_segment, pair_margin):
    seg_ids = jnp.arange(2 * pair_margin.shape[0], dtype=jnp.int32)
    pair_weight = dpo_beta * jax.nn.sigmoid(-dpo_beta * pair_margin)
    table = jnp.repeat(pair_weight, 2) * jnp.where(seg_ids % 2 == 0, -1.0, 1.0).astype(jnp.float32)
    return jnp.sum(
        jnp.where(pol_segment[:, None] == seg_ids[None, :], table[None, :], jnp.float32(0.0)),
        axis=1,
    )


def swap_pairs(n_fsdp, n_tp):
    r = n_tp // n_fsdp
    return [
        (f * n_tp + q * r + j, q * n_tp + f * r + j)
        for f in range(n_fsdp)
        for q in range(n_fsdp)
        for j in range(r)
    ]


def gather_modality(ref_modality, pol_modality, n_fsdp):
    own = jnp.stack([ref_modality, pol_modality])
    me = lax.axis_index("fsdp")
    both = jnp.zeros((n_fsdp,) + own.shape, own.dtype)
    both = lax.dynamic_update_index_in_dim(both, own, me, 0)
    for s in range(1, n_fsdp):
        got = lax.ppermute(own, "fsdp", [(i, (i + s) % n_fsdp) for i in range(n_fsdp)])
        both = lax.dynamic_update_index_in_dim(both, got, (me - s) % n_fsdp, 0)
    return both[:, 0].reshape(-1), both[:, 1].reshape(-1)


def per_device(
    n_fsdp,
    n_tp,
    ref_gate,
    ref_up,
    ref_residual,
    ref_modality,
    ref_down_text,
    ref_down_image,
    pol_gate,
    pol_up,
    pol_modality,
    pol_segment,
    pair_margin,
    token_cotangent,
    pol_down_text,
    pol_down_image,
):
    rows, feats = token_cotangent.shape
    pairs = swap_pairs(n_fsdp, n_tp)
    partner = [(t, t ^ 1) for t in range(n_tp)]
    index = lax.axis_index("tp")
    line, half = index // 2, index % 2

    def shift(step):
        return [(t, (t + 2 * step) % n_tp) for t in range(n_tp)]

    coef = coef_of(pol_segment, pair_margin)
    pol_own = hidden_of(pol_gate, pol_up)
    pol_hidden = lax.all_gather(pol_own, "fsdp", axis=0, tiled=True)
    ref_own = hidden_of(ref_gate, ref_up)
    ref_hidden = lax.all_gather(ref_own, "fsdp", axis=0, tiled=True)

    local_cot = (coef[:, None] * token_cotangent.astype(jnp.float32)).astype(jnp.bfloat16)
    moved = lax.ppermute(local_cot, ("fsdp", "tp"), pairs)
    modality_r, modality_p = gather_modality(ref_modality, pol_modality, n_fsdp)
    image_r = (modality_r == 1)[:, None]
    image_p = (modality_p == 1)[:, None]

    mine = jnp.zeros((n_fsdp, rows, feats), jnp.bfloat16)
    mine = lax.dynamic_update_index_in_dim(mine, moved, line, 0)
    for s in range(1, n_fsdp):
        got = lax.ppermute(moved, "tp", shift(s))
        mine = lax.dynamic_update_index_in_dim(mine, got, (line - s) % n_fsdp, 0)
    mine = mine.reshape(n_fsdp * rows, feats)
    theirs = lax.ppermute(mine, "tp", partner)
    first = half == 0
    cot_full = jnp.concatenate(
        [jnp.where(first, mine, theirs), jnp.where(first, theirs, mine)], axis=1
    )

    dh_text = jnp.dot(cot_full, pol_down_text, preferred_element_type=jnp.float32)
    dh_image = jnp.dot(cot_full, pol_down_image, preferred_element_type=jnp.float32)
    dh_part = jnp.where(image_p, dh_image, dh_text).astype(jnp.bfloat16)
    d_hidden = lax.psum_scatter(dh_part, "fsdp", scatter_dimension=0, tiled=True)

    zero = jnp.zeros_like(cot_full)
    over_rows = (((0,), (0,)), ((), ()))
    g_text = lax.dot_general(
        jnp.where(image_p, zero, cot_full), pol_hidden, over_rows, preferred_element_type=jnp.float32
    )
    g_image = lax.dot_general(
        jnp.where(image_p, cot_full, zero), pol_hidden, over_rows, preferred_element_type=jnp.float32
    )

    contract = (((1,), (1,)), ((), ()))

    def out_half(which):
        w_text = lax.dynamic_slice_in_dim(ref_down_text, which * feats, feats, 0)
        w_image = lax.dynamic_slice_in_dim(ref_down_image, which * feats, feats, 0)
        o_text = lax.dot_general(ref_hidden, w_text, contract, preferred_element_type=jnp.float32)
        o_image = lax.dot_general(ref_hidden, w_image, contract, preferred_element_type=jnp.float32)
        return jnp.where(image_r, o_image, o_text).astype(jnp.bfloat16)

    got = lax.ppermute(out_half(1 - half), "tp", partner)
    keep = out_half(half)
    both = (keep.astype(jnp.float32) + got.astype(jnp.float32)).astype(jnp.bfloat16)
    both = both.reshape(n_fsdp, rows, feats)
    total = lax.dynamic_index_in_dim(both, line, 0, keepdims=False).astype(jnp.float32)
    for s in range(1, n_fsdp):
        piece = lax.dynamic_index_in_dim(both, (line + s) % n_fsdp, 0, keepdims=False)
        total = total + lax.ppermute(piece, "tp", shift(s)).astype(jnp.float32)
    summed = lax.ppermute(total.astype(jnp.bfloat16), ("fsdp", "tp"), pairs)
    ref_out = (summed.astype(jnp.float32) + ref_residual.astype(jnp.float32)).astype(jnp.bfloat16)

    late_gate, late_up, d_hidden = lax.optimization_barrier((pol_gate, pol_up, d_hidden))
    gate_f, up_f, sig, act = silu_parts(late_gate, late_up)
    d_hidden = d_hidden.astype(jnp.float32)
    grad_gate = (d_hidden * up_f * sig * (1.0 + gate_f * (1.0 - sig))).astype(jnp.bfloat16)
    grad_up = (d_hidden * act).astype(jnp.bfloat16)
    return (ref_out, grad_gate, grad_up, g_text, g_image)


def square_kernel(
    ref_gate, ref_up, mod_in, cot_in, ref_text, ref_image, pol_gate, pol_up, pol_text, pol_image,
    out_o, dh_own, dh_x, dh_y, hp_far, gt_o, gi_o, cot_far, mod_far,
    href, hpv, mod, abuf, cot, w, sis_send, sis_recv, zs, zr, fin, rb, dsend, drecv, gtile,
    ss, rs, ls, gs,
):
    n = cot.shape[1]
    rows, half = cot.shape[2], cot.shape[3]
    q = rows // n
    ff = href.shape[1]
    mid = ff // 2
    wide = 2 * LANES
    chunks = rows // wide
    f, t = lax.axis_index("fsdp"), lax.axis_index("tp")
    z, c = t // 2, t % 2
    oc = 1 - c
    fs = (f, f + 1 - 2 * (f % 2), (f + 2) % n, n - 1 - f)
    zp = [(z + r) % n for r in range(n)]
    zm = [(z + n - r) % n for r in range(n)]
    side = [(fs[s], t) for s in range(4)]
    up = [(f, 2 * zp[r] + c) for r in range(n)]
    sister = (f, 2 * z + oc)
    count = [0]
    lcount = [0]
    sends = []

    def remote(src, dst, dev):
        i = count[0]
        count[0] += 1
        copy = pltpu.make_async_remote_copy(
            src_ref=src, dst_ref=dst, send_sem=ss.at[i], recv_sem=rs.at[i],
            device_id=dev, device_id_type=MESH,
        )
        copy.start()
        sends.append(copy)
        return copy

    def local(src, dst):
        i = lcount[0]
        lcount[0] += 1
        copy = pltpu.make_async_copy(src, dst, ls.at[i])
        copy.start()
        return copy

    def piece(i):
        return pl.ds(pl.multiple_of(i * q, q), q)

    top, low = pl.ds(0, mid), pl.ds(mid, mid)
    loads = [
        [local(src.at[part], dsend.at[i, part]) for i, src in ((0, ref_gate), (1, ref_up))]
        for part in (top, low)
    ]
    a_own = local(cot_in.at[piece(z)], abuf.at[z])
    mod_own = local(mod_in, mod.at[0])
    w_ld = [local(ref_text, w.at[0]), local(ref_image, w.at[1])]
    pol_ld = [local(pol_gate, dsend.at[2]), local(pol_up, dsend.at[3])]

    barrier = pltpu.get_barrier_semaphore()
    peers = [side[1], side[2], side[3]] + [up[r] for r in range(1, n)] + [sister]
    for peer in peers:
        pl.semaphore_signal(barrier, inc=1, device_id=peer, device_id_type=MESH)
    pl.semaphore_wait(barrier, len(peers))

    a_cp = [remote(cot_in.at[piece(zp[r])], abuf.at[z], up[r]) for r in range(1, n)]
    m_cp = [remote(mod_in, mod.at[s], side[s]) for s in range(1, 4)]

    def hidden_rows(first, src, dst):
        @pl.loop(0, mid // 16)
        def _(i):
            at = pl.ds(pl.multiple_of(first + i * 16, 16), 16)
            gate = dsend[src, at, :].astype(jnp.float32)
            act = gate * jax.nn.sigmoid(gate)
            dst[0, at, :] = (act * dsend[src + 1, at, :].astype(jnp.float32)).astype(jnp.bfloat16)

    for copy in loads[0]:
        copy.wait()
    hidden_rows(0, 0, href)
    own_x = [remote(href.at[0, top], href.at[1, top], side[1])]
    for copy in loads[1]:
        copy.wait()
    hidden_rows(mid, 0, href)
    own_y = [remote(href.at[0, low], href.at[2, low], side[2])]
    for copy in pol_ld:
        copy.wait()
    hidden_rows(0, 2, hpv)
    hidden_rows(mid, 2, hpv)

    a_own.wait()
    for copy in a_cp:
        copy.wait_recv()
    b_cp = [remote(abuf.at[fs[s]], cot.at[c, s, piece(z)], side[s]) for s in range(1, 4)]
    own_x.append(remote(href.at[0, low], href.at[1, low], side[1]))
    own_y.append(remote(href.at[0, top], href.at[2, top], side[2]))
    cot[c, 0, piece(z), :] = abuf[f]

    def lanes(j, size):
        return pl.ds(pl.multiple_of(j * size, size), size)

    over_ff = (((0,), (0,)), ((), ()))

    def out_rows(s, j, which):
        cols = lanes(which, half)
        image = mod[s, :, lanes(j, wide)][0:1]
        h = href[s, :, lanes(j, wide)]
        h_image = h * image
        h_text = h * (1.0 - image)
        o_text = lax.dot_general(h_text, w[0, :, cols], over_ff, preferred_element_type=jnp.float32)
        o_image = lax.dot_general(h_image, w[1, :, cols], over_ff, preferred_element_type=jnp.float32)
        return o_text + o_image

    e_cp = {}
    f_cp = []

    def out_other(s):
        @pl.loop(0, chunks)
        def _(j):
            sis_send[s, lanes(j, wide), :] = out_rows(s, j, oc).astype(jnp.bfloat16)

        e_cp[s] = remote(sis_send.at[s], sis_recv.at[s], sister)

    def out_own(s):
        e_cp[s].wait_recv()

        @pl.loop(0, chunks)
        def _(j):
            total = out_rows(s, j, c) + sis_recv[s, lanes(j, wide), :].astype(jnp.float32)
            zs[s, lanes(j, wide), :] = total.astype(jnp.bfloat16)

        for r in range(1, n):
            f_cp.append(remote(zs.at[s, piece(zp[r])], zr.at[r - 1, s], up[r]))

    mod_own.wait()
    for copy in w_ld:
        copy.wait()
    out_other(0)
    for copy in b_cp:
        copy.wait_recv()
    c_cp = [remote(cot.at[c, :, piece(z)], cot.at[c, :, piece(z)], up[r]) for r in range(1, n)]
    d_cp = [remote(cot.at[c, :, piece(z)], cot.at[c, :, piece(z)], sister)]
    own_x[0].wait_recv()
    fwd_y = remote(href.at[1, top], href.at[3, top], side[2])
    own_y[0].wait_recv()
    fwd_x = remote(href.at[2, low], href.at[3, low], side[1])
    out_own(0)
    pol_x = [remote(hpv.at[0, part], hpv.at[1, part], side[1]) for part in (top, low)]
    pol_y = [remote(hpv.at[0, part], hpv.at[2, part], side[2]) for part in (low, top)]
    for copy in m_cp:
        copy.wait_recv()
    own_x[1].wait_recv()
    own_y[1].wait_recv()
    out_other(1)
    out_other(2)
    out_own(1)
    out_own(2)
    fwd_y.wait_recv()
    fwd_x.wait_recv()
    mod_cp = local(mod.at[3], mod_far)
    out_other(3)
    for r in range(1, n):
        c_cp[r - 1].wait_recv()
        d_cp.append(remote(cot.at[c, :, piece(zm[r])], cot.at[c, :, piece(zm[r])], sister))
    out_own(3)
    w_ld = [local(pol_text, w.at[0]), local(pol_image, w.at[1])]
    for copy in d_cp:
        copy.wait_recv()
    for copy in w_ld:
        copy.wait()
    far_cp = [local(cot.at[h, 3], cot_far.at[:, pl.ds(h * half, half)]) for h in range(2)]

    over_last = (((1,), (1,)), ((), ()))

    def dh_part(s, first, got):
        part = pl.ds(first, mid)

        @pl.loop(0, chunks)
        def _(j):
            at = lanes(j, wide)

            def of(i):
                lo = lax.dot_general(
                    w[i, part, :half], cot[0, s, at, :], over_last, preferred_element_type=jnp.float32
                )
                return lo + lax.dot_general(
                    w[i, part, half:], cot[1, s, at, :], over_last, preferred_element_type=jnp.float32
                )

            row = mod[s, :, at].astype(jnp.float32)[1:2]
            image = jnp.broadcast_to(row, (mid, wide)) > 0.5
            d = jnp.where(image, of(1), of(0))
            if got is not None:
                d = d + drecv[got, :, at].astype(jnp.float32)
            dsend[s, part, at] = d.astype(jnp.bfloat16)

    dh_part(3, 0, None)
    i_x = remote(dsend.at[3, top], drecv.at[0], side[1])
    dh_part(3, mid, None)
    i_y = remote(dsend.at[3, low], drecv.at[1], side[2])
    dh_part(1, 0, None)
    j_cp = [remote(dsend.at[1, top], dh_x.at[top], side[1])]
    dh_part(2, mid, None)
    j_cp.append(remote(dsend.at[2, low], dh_y.at[low], side[2]))
    for copy in pol_x + pol_y:
        copy.wait_recv()
    polf_y = remote(hpv.at[1, top], hp_far.at[top], side[2])
    polf_x = remote(hpv.at[2, low], hp_far.at[low], side[1])
    dh_part(0, 0, None)
    dh_part(0, mid, None)
    own_cp = local(dsend.at[0], dh_own)

    per_half = half // wide
    tiles = 2 * per_half

    def g_copies(i):
        slot, a, j = i % 2, i // tiles, i % tiles
        at = pl.ds(pl.multiple_of(a * mid, mid), mid)
        return (
            pltpu.make_async_copy(gtile.at[slot, 0], gt_o.at[at, lanes(j, wide)], gs.at[slot, 0]),
            pltpu.make_async_copy(gtile.at[slot, 1], gi_o.at[at, lanes(j, wide)], gs.at[slot, 1]),
        )

    @pl.loop(0, 2 * tiles)
    def _(i):
        a, j = i // tiles, i % tiles
        at = pl.ds(pl.multiple_of(a * mid, mid), mid)
        g_text, g_image = None, None
        for s in range(3):
            y = cot[j // per_half, s, :, lanes(j % per_half, wide)]
            image = mod[s][1:2]
            h = hpv[s, at, :]
            t_text = jnp.dot(h * (1.0 - image), y, preferred_element_type=jnp.float32)
            t_image = jnp.dot(h * image, y, preferred_element_type=jnp.float32)
            g_text = t_text if g_text is None else g_text + t_text
            g_image = t_image if g_image is None else g_image + t_image

        @pl.when(i >= 2)
        def _():
            for copy in g_copies(i - 2):
                copy.wait()

        gtile[i % 2, 0] = g_text
        gtile[i % 2, 1] = g_image
        for copy in g_copies(i):
            copy.start()

    i_y.wait_recv()
    dh_part(1, mid, 1)
    i_x.wait_recv()
    dh_part(2, 0, 0)

    for copy in f_cp:
        copy.wait_recv()
    for s in range(4):
        total = zs[s, piece(z), :].astype(jnp.float32)
        for r in range(1, n):
            total = total + zr[r - 1, s].astype(jnp.float32)
        fin[s] = total.astype(jnp.bfloat16)
    rb[f] = fin[0]
    g_cp = [remote(fin.at[s], rb.at[f], side[s]) for s in range(1, 4)]
    j_cp.append(remote(dsend.at[1, low], dh_x.at[low], side[1]))
    j_cp.append(remote(dsend.at[2, top], dh_y.at[top], side[2]))
    for copy in g_cp:
        copy.wait_recv()
    h_cp = [remote(rb.at[zp[r]], out_o.at[piece(z)], up[r]) for r in range(1, n)]
    h_own = local(rb.at[z], out_o.at[piece(z)])
    for i in (2 * tiles - 2, 2 * tiles - 1):
        for copy in g_copies(i):
            copy.wait()
    for copy in [h_own, own_cp, mod_cp] + far_cp:
        copy.wait()
    for copy in h_cp + [polf_x, polf_y] + j_cp:
        copy.wait_recv()
    for copy in sends:
        copy.wait_send()


def square_per_device(
    n_fsdp,
    n_tp,
    ref_gate,
    ref_up,
    ref_residual,
    ref_modality,
    ref_down_text,
    ref_down_image,
    pol_gate,
    pol_up,
    pol_modality,
    pol_segment,
    pair_margin,
    token_cotangent,
    pol_down_text,
    pol_down_image,
):
    rows, feats = token_cotangent.shape
    ff = ref_gate.shape[1]
    n = n_fsdp
    q = rows // n
    bf16 = jnp.bfloat16
    coef = coef_of(pol_segment, pair_margin)
    cot_in = (coef[:, None] * token_cotangent.astype(jnp.float32)).astype(bf16)
    row = lax.broadcasted_iota(jnp.int32, (16, rows), 0)
    mod_in = jnp.where(row == 0, ref_modality[None, :], jnp.where(row == 1, pol_modality[None, :], 0))
    mod_in = mod_in.astype(bf16)

    shape = jax.ShapeDtypeStruct
    block = shape((ff, rows), bf16)
    grad = shape((ff, 2 * feats), jnp.float32)
    anywhere = pl.BlockSpec(memory_space=pl.ANY)
    outs = (
        shape((rows, feats), bf16), block, block, block, block, grad, grad,
        shape((rows, 2 * feats), bf16), shape((16, rows), bf16),
    )
    scratch = [
        pltpu.VMEM((4, ff, rows), bf16),
        pltpu.VMEM((3, ff, rows), bf16),
        pltpu.VMEM((4, 16, rows), bf16),
        pltpu.VMEM((n, q, feats), bf16),
        pltpu.VMEM((2, 4, rows, feats), bf16),
        pltpu.VMEM((2, ff, 2 * feats), bf16),
        pltpu.VMEM((4, rows, feats), bf16),
        pltpu.VMEM((4, rows, feats), bf16),
        pltpu.VMEM((4, rows, feats), bf16),
        pltpu.VMEM((n - 1, 4, q, feats), bf16),
        pltpu.VMEM((4, q, feats), bf16),
        pltpu.VMEM((4, q, feats), bf16),
        pltpu.VMEM((4, ff, rows), bf16),
        pltpu.VMEM((2, ff // 2, rows), bf16),
        pltpu.VMEM((2, 2, ff // 2, 2 * LANES), jnp.float32),
        pltpu.SemaphoreType.DMA((64,)),
        pltpu.SemaphoreType.DMA((64,)),
        pltpu.SemaphoreType.DMA((24,)),
        pltpu.SemaphoreType.DMA((2, 2)),
    ]
    out, own, from_x, from_y, hp_far, g_text, g_image, cot_far, mod_far = pl.pallas_call(
        square_kernel,
        out_shape=outs,
        in_specs=[anywhere] * 10,
        out_specs=(anywhere,) * len(outs),
        scratch_shapes=scratch,
        compiler_params=pltpu.CompilerParams(
            collective_id=0, has_side_effects=True, vmem_limit_bytes=VMEM_BYTES
        ),
        name="square_step",
    )(
        ref_gate.T, ref_up.T, mod_in, cot_in, ref_down_text.T, ref_down_image.T,
        pol_gate.T, pol_up.T, pol_down_text.T, pol_down_image.T,
    )

    ref_out = (out.astype(jnp.float32) + ref_residual.astype(jnp.float32)).astype(bf16)

    gate_f, up_f, sig, act = silu_parts(pol_gate.T, pol_up.T)
    d_hidden = own.astype(jnp.float32) + from_x.astype(jnp.float32) + from_y.astype(jnp.float32)
    grad_gate = (d_hidden * up_f * sig * (1.0 + gate_f * (1.0 - sig))).astype(bf16)
    grad_up = (d_hidden * act).astype(bf16)

    image = mod_far[1:2] > 0.5
    zero = jnp.zeros_like(hp_far)
    g_text = g_text + jnp.dot(jnp.where(image, zero, hp_far), cot_far, preferred_element_type=jnp.float32)
    g_image = g_image + jnp.dot(jnp.where(image, hp_far, zero), cot_far, preferred_element_type=jnp.float32)
    return (ref_out, grad_gate.T, grad_up.T, g_text.T, g_image.T)


def solution(mesh):
    n_fsdp, n_tp = mesh.shape["fsdp"], mesh.shape["tp"]
    two = P("fsdp", "tp")
    one = P("fsdp")
    in_specs = (two, two, two, one, two, two, two, two, one, one, P(), two, two, two)
    square = n_fsdp == 4 and n_tp == 2 * n_fsdp
    plan = square_per_device if square else per_device

    def body(*args):
        return plan(n_fsdp, n_tp, *args)

    return jax.shard_map(
        body, mesh=mesh, in_specs=in_specs, out_specs=(two,) * 5, check_vma=False
    )
```

```python
import jax
import jax.numpy as jnp
from jax import lax
from jax.experimental import pallas as pl
from jax.experimental.pallas import tpu as pltpu
from jax.sharding import PartitionSpec as P


MESH = pl.DeviceIdType.MESH
LANES = 128
VMEM_BYTES = 67043328

dpo_beta = 0.1


def silu_parts(gate, up):
    gate_f = gate.astype(jnp.float32)
    up_f = up.astype(jnp.float32)
    sig = jax.nn.sigmoid(gate_f)
    act = gate_f * sig
    return gate_f, up_f, sig, act


def hidden_of(gate, up):
    _, up_f, _, act = silu_parts(gate, up)
    return (act * up_f).astype(jnp.bfloat16)


def coef_of(pol_segment, pair_margin):
    seg_ids = jnp.arange(2 * pair_margin.shape[0], dtype=jnp.int32)
    pair_weight = dpo_beta * jax.nn.sigmoid(-dpo_beta * pair_margin)
    table = jnp.repeat(pair_weight, 2) * jnp.where(seg_ids % 2 == 0, -1.0, 1.0).astype(jnp.float32)
    return jnp.sum(
        jnp.where(pol_segment[:, None] == seg_ids[None, :], table[None, :], jnp.float32(0.0)),
        axis=1,
    )


def swap_pairs(n_fsdp, n_tp):
    r = n_tp // n_fsdp
    return [
        (f * n_tp + q * r + j, q * n_tp + f * r + j)
        for f in range(n_fsdp)
        for q in range(n_fsdp)
        for j in range(r)
    ]


def gather_modality(ref_modality, pol_modality, n_fsdp):
    own = jnp.stack([ref_modality, pol_modality])
    me = lax.axis_index("fsdp")
    both = jnp.zeros((n_fsdp,) + own.shape, own.dtype)
    both = lax.dynamic_update_index_in_dim(both, own, me, 0)
    for s in range(1, n_fsdp):
        got = lax.ppermute(own, "fsdp", [(i, (i + s) % n_fsdp) for i in range(n_fsdp)])
        both = lax.dynamic_update_index_in_dim(both, got, (me - s) % n_fsdp, 0)
    return both[:, 0].reshape(-1), both[:, 1].reshape(-1)


def per_device(
    n_fsdp,
    n_tp,
    ref_gate,
    ref_up,
    ref_residual,
    ref_modality,
    ref_down_text,
    ref_down_image,
    pol_gate,
    pol_up,
    pol_modality,
    pol_segment,
    pair_margin,
    token_cotangent,
    pol_down_text,
    pol_down_image,
):
    rows, feats = token_cotangent.shape
    pairs = swap_pairs(n_fsdp, n_tp)
    partner = [(t, t ^ 1) for t in range(n_tp)]
    index = lax.axis_index("tp")
    line, half = index // 2, index % 2

    def shift(step):
        return [(t, (t + 2 * step) % n_tp) for t in range(n_tp)]

    coef = coef_of(pol_segment, pair_margin)
    pol_own = hidden_of(pol_gate, pol_up)
    pol_hidden = lax.all_gather(pol_own, "fsdp", axis=0, tiled=True)
    ref_own = hidden_of(ref_gate, ref_up)
    ref_hidden = lax.all_gather(ref_own, "fsdp", axis=0, tiled=True)

    local_cot = (coef[:, None] * token_cotangent.astype(jnp.float32)).astype(jnp.bfloat16)
    moved = lax.ppermute(local_cot, ("fsdp", "tp"), pairs)
    modality_r, modality_p = gather_modality(ref_modality, pol_modality, n_fsdp)
    image_r = (modality_r == 1)[:, None]
    image_p = (modality_p == 1)[:, None]

    mine = jnp.zeros((n_fsdp, rows, feats), jnp.bfloat16)
    mine = lax.dynamic_update_index_in_dim(mine, moved, line, 0)
    for s in range(1, n_fsdp):
        got = lax.ppermute(moved, "tp", shift(s))
        mine = lax.dynamic_update_index_in_dim(mine, got, (line - s) % n_fsdp, 0)
    mine = mine.reshape(n_fsdp * rows, feats)
    theirs = lax.ppermute(mine, "tp", partner)
    first = half == 0
    cot_full = jnp.concatenate(
        [jnp.where(first, mine, theirs), jnp.where(first, theirs, mine)], axis=1
    )

    dh_text = jnp.dot(cot_full, pol_down_text, preferred_element_type=jnp.float32)
    dh_image = jnp.dot(cot_full, pol_down_image, preferred_element_type=jnp.float32)
    dh_part = jnp.where(image_p, dh_image, dh_text).astype(jnp.bfloat16)
    d_hidden = lax.psum_scatter(dh_part, "fsdp", scatter_dimension=0, tiled=True)

    zero = jnp.zeros_like(cot_full)
    over_rows = (((0,), (0,)), ((), ()))
    g_text = lax.dot_general(
        jnp.where(image_p, zero, cot_full), pol_hidden, over_rows, preferred_element_type=jnp.float32
    )
    g_image = lax.dot_general(
        jnp.where(image_p, cot_full, zero), pol_hidden, over_rows, preferred_element_type=jnp.float32
    )

    contract = (((1,), (1,)), ((), ()))

    def out_half(which):
        w_text = lax.dynamic_slice_in_dim(ref_down_text, which * feats, feats, 0)
        w_image = lax.dynamic_slice_in_dim(ref_down_image, which * feats, feats, 0)
        o_text = lax.dot_general(ref_hidden, w_text, contract, preferred_element_type=jnp.float32)
        o_image = lax.dot_general(ref_hidden, w_image, contract, preferred_element_type=jnp.float32)
        return jnp.where(image_r, o_image, o_text).astype(jnp.bfloat16)

    got = lax.ppermute(out_half(1 - half), "tp", partner)
    keep = out_half(half)
    both = (keep.astype(jnp.float32) + got.astype(jnp.float32)).astype(jnp.bfloat16)
    both = both.reshape(n_fsdp, rows, feats)
    total = lax.dynamic_index_in_dim(both, line, 0, keepdims=False).astype(jnp.float32)
    for s in range(1, n_fsdp):
        piece = lax.dynamic_index_in_dim(both, (line + s) % n_fsdp, 0, keepdims=False)
        total = total + lax.ppermute(piece, "tp", shift(s)).astype(jnp.float32)
    summed = lax.ppermute(total.astype(jnp.bfloat16), ("fsdp", "tp"), pairs)
    ref_out = (summed.astype(jnp.float32) + ref_residual.astype(jnp.float32)).astype(jnp.bfloat16)

    late_gate, late_up, d_hidden = lax.optimization_barrier((pol_gate, pol_up, d_hidden))
    gate_f, up_f, sig, act = silu_parts(late_gate, late_up)
    d_hidden = d_hidden.astype(jnp.float32)
    grad_gate = (d_hidden * up_f * sig * (1.0 + gate_f * (1.0 - sig))).astype(jnp.bfloat16)
    grad_up = (d_hidden * act).astype(jnp.bfloat16)
    return (ref_out, grad_gate, grad_up, g_text, g_image)


def square_kernel(
    margin, ref_gate, ref_up, residual, ref_mod, ref_text, ref_image, pol_gate, pol_up, pol_mod, pol_seg, cot_raw,
    pol_text, pol_image,
    out_o, gg_o, gu_o, gt_o, gi_o,
    href, hpv, tags, mod, own_cot, abuf, cot, w, sis_send, sis_recv, zs, zr, fin, rb, ra, dsend, drecv, dxy, gtile,
    ss, rs, ls, gs,
):
    n = cot.shape[1]
    rows, half = cot.shape[2], cot.shape[3]
    q = rows // n
    ff = href.shape[1]
    mid = ff // 2
    wide = 2 * LANES
    chunks = rows // wide
    f, t = lax.axis_index("fsdp"), lax.axis_index("tp")
    z, c = t // 2, t % 2
    oc = 1 - c
    fs = (f, f + 1 - 2 * (f % 2), (f + 2) % n, n - 1 - f)
    zp = [(z + r) % n for r in range(n)]
    zm = [(z + n - r) % n for r in range(n)]
    side = [(fs[s], t) for s in range(4)]
    up = [(f, 2 * zp[r] + c) for r in range(n)]
    sister = (f, 2 * z + oc)
    count = [0]
    lcount = [0]
    sends = []

    def remote(src, dst, dev):
        i = count[0]
        count[0] += 1
        copy = pltpu.make_async_remote_copy(
            src_ref=src, dst_ref=dst, send_sem=ss.at[i], recv_sem=rs.at[i],
            device_id=dev, device_id_type=MESH,
        )
        copy.start()
        sends.append(copy)
        return copy

    def local(src, dst):
        i = lcount[0]
        lcount[0] += 1
        copy = pltpu.make_async_copy(src, dst, ls.at[i])
        copy.start()
        return copy

    def piece(i):
        return pl.ds(pl.multiple_of(i * q, q), q)

    top, low = pl.ds(0, mid), pl.ds(mid, mid)
    loads = [
        [local(src.at[part], dsend.at[i, part]) for i, src in ((0, ref_gate), (1, ref_up))]
        for part in (top, low)
    ]
    small = [local(src, tags.at[i]) for i, src in enumerate((ref_mod, pol_mod, pol_seg))]
    small.append(local(cot_raw, own_cot))
    w_ld = [local(ref_text, w.at[0]), local(ref_image, w.at[1])]
    pol_ld = [local(pol_gate, dsend.at[2]), local(pol_up, dsend.at[3])]

    barrier = pltpu.get_barrier_semaphore()
    peers = [side[1], side[2], side[3]] + [up[r] for r in range(1, n)] + [sister]
    for peer in peers:
        pl.semaphore_signal(barrier, inc=1, device_id=peer, device_id_type=MESH)
    pl.semaphore_wait(barrier, len(peers))

    def hidden_rows(first, src, dst):
        @pl.loop(0, mid // 16)
        def _(i):
            at = pl.ds(pl.multiple_of(first + i * 16, 16), 16)
            gate = dsend[src, at, :].astype(jnp.float32)
            act = gate * jax.nn.sigmoid(gate)
            dst[0, at, :] = (act * dsend[src + 1, at, :].astype(jnp.float32)).astype(jnp.bfloat16)

    for copy in loads[0]:
        copy.wait()
    hidden_rows(0, 0, href)
    own_x = [remote(href.at[0, top], href.at[1, top], side[1])]
    for copy in loads[1]:
        copy.wait()
    hidden_rows(mid, 0, href)
    own_y = [remote(href.at[0, low], href.at[2, low], side[2])]
    for copy in small:
        copy.wait()

    def tag_row(i, size):
        return jnp.concatenate(
            [jnp.broadcast_to(tags[i, j : j + 1, :], (size, LANES)) for j in range(rows // LANES)], axis=1
        )

    seg = tag_row(2, 8)
    coef = jnp.zeros((8, rows), jnp.float32)
    for p in range(margin.shape[0]):
        weight = dpo_beta * jax.nn.sigmoid(-dpo_beta * jnp.full((8, rows), margin[p], jnp.float32))
        coef = jnp.where(seg // 2 == p, weight, coef)
    coef = jnp.where(seg % 2 == 0, -coef, coef).T[:, 0:1]
    own_cot[...] = (coef * own_cot[...].astype(jnp.float32)).astype(jnp.bfloat16)
    row = lax.broadcasted_iota(jnp.int32, (16, rows), 0)
    both = jnp.where(row == 0, tag_row(0, 16), jnp.where(row == 1, tag_row(1, 16), 0))
    mod[0] = both.astype(jnp.float32).astype(jnp.bfloat16)
    a_cp = [remote(own_cot.at[piece(zp[r])], abuf.at[z], up[r]) for r in range(1, n)]
    m_cp = [remote(mod.at[0], mod.at[s], side[s]) for s in range(1, 4)]
    abuf[z] = own_cot[piece(z), :]
    for copy in pol_ld:
        copy.wait()
    hidden_rows(0, 2, hpv)
    hidden_rows(mid, 2, hpv)

    for copy in a_cp:
        copy.wait_recv()
    b_cp = [remote(abuf.at[fs[s]], cot.at[c, s, piece(z)], side[s]) for s in range(1, 4)]
    own_x.append(remote(href.at[0, low], href.at[1, low], side[1]))
    own_y.append(remote(href.at[0, top], href.at[2, top], side[2]))
    cot[c, 0, piece(z), :] = abuf[f]

    def lanes(j, size):
        return pl.ds(pl.multiple_of(j * size, size), size)

    over_ff = (((0,), (0,)), ((), ()))

    def out_rows(s, j, which):
        cols = lanes(which, half)
        image = mod[s, :, lanes(j, wide)][0:1]
        h = href[s, :, lanes(j, wide)]
        h_image = h * image
        h_text = h * (1.0 - image)
        o_text = lax.dot_general(h_text, w[0, :, cols], over_ff, preferred_element_type=jnp.float32)
        o_image = lax.dot_general(h_image, w[1, :, cols], over_ff, preferred_element_type=jnp.float32)
        return o_text + o_image

    e_cp = {}
    f_cp = []

    def out_other(s):
        @pl.loop(0, chunks)
        def _(j):
            sis_send[s, lanes(j, wide), :] = out_rows(s, j, oc).astype(jnp.bfloat16)

        e_cp[s] = remote(sis_send.at[s], sis_recv.at[s], sister)

    def out_own(s):
        e_cp[s].wait_recv()

        @pl.loop(0, chunks)
        def _(j):
            total = out_rows(s, j, c) + sis_recv[s, lanes(j, wide), :].astype(jnp.float32)
            zs[s, lanes(j, wide), :] = total.astype(jnp.bfloat16)

        for r in range(1, n):
            f_cp.append(remote(zs.at[s, piece(zp[r])], zr.at[r - 1, s], up[r]))

    for copy in w_ld:
        copy.wait()
    out_other(0)
    for copy in b_cp:
        copy.wait_recv()
    c_cp = [remote(cot.at[c, :, piece(z)], cot.at[c, :, piece(z)], up[r]) for r in range(1, n)]
    d_cp = [remote(cot.at[c, :, piece(z)], cot.at[c, :, piece(z)], sister)]
    own_x[0].wait_recv()
    fwd_y = remote(href.at[1, top], href.at[3, top], side[2])
    own_y[0].wait_recv()
    fwd_x = remote(href.at[2, low], href.at[3, low], side[1])
    out_own(0)
    pol_x = [remote(hpv.at[0, part], hpv.at[1, part], side[1]) for part in (top, low)]
    pol_y = [remote(hpv.at[0, part], hpv.at[2, part], side[2]) for part in (low, top)]
    for copy in m_cp:
        copy.wait_recv()
    own_x[1].wait_recv()
    own_y[1].wait_recv()
    out_other(1)
    out_other(2)
    out_own(1)
    out_own(2)
    fwd_y.wait_recv()
    fwd_x.wait_recv()
    out_other(3)
    out_own(3)
    pol_x[0].wait_recv()
    polf_y = remote(hpv.at[1, top], hpv.at[3, top], side[2])
    pol_y[0].wait_recv()
    polf_x = remote(hpv.at[2, low], hpv.at[3, low], side[1])
    for r in range(1, n):
        c_cp[r - 1].wait_recv()
        d_cp.append(remote(cot.at[c, :, piece(zm[r])], cot.at[c, :, piece(zm[r])], sister))
    w_ld = [local(pol_text, w.at[0]), local(pol_image, w.at[1])]
    for copy in d_cp:
        copy.wait_recv()
    for copy in w_ld:
        copy.wait()
    waited = own_x + own_y + [fwd_x, fwd_y] + a_cp
    for copy in waited:
        copy.wait_send()
    gate_ld = [local(pol_gate, href.at[0]), local(pol_up, href.at[1]), local(residual, own_cot)]

    over_last = (((1,), (1,)), ((), ()))

    def dh_part(s, first, got):
        part = pl.ds(first, mid)

        @pl.loop(0, chunks)
        def _(j):
            at = lanes(j, wide)

            def of(i):
                lo = lax.dot_general(
                    w[i, part, :half], cot[0, s, at, :], over_last, preferred_element_type=jnp.float32
                )
                return lo + lax.dot_general(
                    w[i, part, half:], cot[1, s, at, :], over_last, preferred_element_type=jnp.float32
                )

            row = mod[s, :, at].astype(jnp.float32)[1:2]
            image = jnp.broadcast_to(row, (mid, wide)) > 0.5
            d = jnp.where(image, of(1), of(0))
            if got is not None:
                d = d + drecv[got, :, at].astype(jnp.float32)
            dsend[s, part, at] = d.astype(jnp.bfloat16)

    dh_part(3, 0, None)
    i_x = remote(dsend.at[3, top], drecv.at[0], side[1])
    dh_part(3, mid, None)
    i_y = remote(dsend.at[3, low], drecv.at[1], side[2])
    dh_part(1, 0, None)
    j_cp = [remote(dsend.at[1, top], dxy.at[0, top], side[1])]
    dh_part(2, mid, None)
    j_cp.append(remote(dsend.at[2, low], dxy.at[1, low], side[2]))
    dh_part(0, 0, None)
    dh_part(0, mid, None)

    for copy in f_cp:
        copy.wait_recv()
    for s in range(4):
        total = zs[s, piece(z), :].astype(jnp.float32)
        for r in range(1, n):
            total = total + zr[r - 1, s].astype(jnp.float32)
        fin[s] = total.astype(jnp.bfloat16)
    rb[f] = fin[0]
    g_cp = [remote(fin.at[s], rb.at[f], side[s]) for s in range(1, 4)]
    i_y.wait_recv()
    dh_part(1, mid, 1)
    j_cp.append(remote(dsend.at[1, low], dxy.at[0, low], side[1]))
    i_x.wait_recv()
    dh_part(2, 0, 0)
    j_cp.append(remote(dsend.at[2, top], dxy.at[1, top], side[2]))

    for copy in [pol_x[1], pol_y[1], polf_x, polf_y]:
        copy.wait_recv()
    per_half = half // wide
    tiles = 2 * per_half

    def g_copies(i):
        slot, a, j = i % 2, i // tiles, i % tiles
        at = pl.ds(pl.multiple_of(a * mid, mid), mid)
        return (
            pltpu.make_async_copy(gtile.at[slot, 0], gt_o.at[at, lanes(j, wide)], gs.at[slot, 0]),
            pltpu.make_async_copy(gtile.at[slot, 1], gi_o.at[at, lanes(j, wide)], gs.at[slot, 1]),
        )

    @pl.loop(0, 2 * tiles)
    def _(i):
        a, j = i // tiles, i % tiles
        at = pl.ds(pl.multiple_of(a * mid, mid), mid)
        g_text, g_image = None, None
        for s in range(4):
            y = cot[j // per_half, s, :, lanes(j % per_half, wide)]
            image = mod[s][1:2]
            h = hpv[s, at, :]
            t_text = jnp.dot(h * (1.0 - image), y, preferred_element_type=jnp.float32)
            t_image = jnp.dot(h * image, y, preferred_element_type=jnp.float32)
            g_text = t_text if g_text is None else g_text + t_text
            g_image = t_image if g_image is None else g_image + t_image

        @pl.when(i >= 2)
        def _():
            for copy in g_copies(i - 2):
                copy.wait()

        gtile[i % 2, 0] = g_text
        gtile[i % 2, 1] = g_image
        for copy in g_copies(i):
            copy.start()

    for copy in g_cp:
        copy.wait_recv()
    h_cp = [remote(rb.at[zp[r]], ra.at[z], up[r]) for r in range(1, n)]
    ra[z] = rb[z]
    for i in (2 * tiles - 2, 2 * tiles - 1):
        for copy in g_copies(i):
            copy.wait()
    for copy in gate_ld:
        copy.wait()
    for copy in h_cp:
        copy.wait_recv()
    total = own_cot[...].astype(jnp.float32) + ra[...].reshape(rows, half).astype(jnp.float32)
    own_cot[...] = total.astype(jnp.bfloat16)
    done = [local(own_cot, out_o)]

    def grad_rows(first):
        @pl.loop(0, mid // 16)
        def _(i):
            at = pl.ds(pl.multiple_of(first + i * 16, 16), 16)
            d = dsend[0, at, :].astype(jnp.float32)
            d = d + dxy[0, at, :].astype(jnp.float32) + dxy[1, at, :].astype(jnp.float32)
            gate, up_f = href[0, at, :].astype(jnp.float32), href[1, at, :].astype(jnp.float32)
            sig = jax.nn.sigmoid(gate)
            href[2, at, :] = (d * up_f * sig * (1.0 + gate * (1.0 - sig))).astype(jnp.bfloat16)
            href[3, at, :] = (d * gate * sig).astype(jnp.bfloat16)

    for first, part, pair in ((0, top, (0, 3)), (mid, low, (1, 2))):
        for i in pair:
            j_cp[i].wait_recv()
        grad_rows(first)
        done += [local(href.at[2, part], gg_o.at[part]), local(href.at[3, part], gu_o.at[part])]
    for copy in sends:
        if all(copy is not other for other in waited):
            copy.wait_send()
    for copy in done:
        copy.wait()


def square_per_device(
    n_fsdp,
    n_tp,
    ref_gate,
    ref_up,
    ref_residual,
    ref_modality,
    ref_down_text,
    ref_down_image,
    pol_gate,
    pol_up,
    pol_modality,
    pol_segment,
    pair_margin,
    token_cotangent,
    pol_down_text,
    pol_down_image,
):
    rows, feats = token_cotangent.shape
    ff = ref_gate.shape[1]
    n = n_fsdp
    q = rows // n
    bf16 = jnp.bfloat16
    shape = jax.ShapeDtypeStruct
    block = shape((ff, rows), bf16)
    grad = shape((ff, 2 * feats), jnp.float32)
    anywhere = pl.BlockSpec(memory_space=pl.ANY)
    outs = (shape((rows, feats), bf16), block, block, grad, grad)
    scratch = [
        pltpu.VMEM((4, ff, rows), bf16),
        pltpu.VMEM((4, ff, rows), bf16),
        pltpu.VMEM((3, rows // LANES, LANES), jnp.int32),
        pltpu.VMEM((4, 16, rows), bf16),
        pltpu.VMEM((rows, feats), bf16),
        pltpu.VMEM((n, q, feats), bf16),
        pltpu.VMEM((2, 4, rows, feats), bf16),
        pltpu.VMEM((2, ff, 2 * feats), bf16),
        pltpu.VMEM((4, rows, feats), bf16),
        pltpu.VMEM((4, rows, feats), bf16),
        pltpu.VMEM((4, rows, feats), bf16),
        pltpu.VMEM((n - 1, 4, q, feats), bf16),
        pltpu.VMEM((4, q, feats), bf16),
        pltpu.VMEM((4, q, feats), bf16),
        pltpu.VMEM((4, q, feats), bf16),
        pltpu.VMEM((4, ff, rows), bf16),
        pltpu.VMEM((2, ff // 2, rows), bf16),
        pltpu.VMEM((2, ff, rows), bf16),
        pltpu.VMEM((2, 2, ff // 2, 2 * LANES), jnp.float32),
        pltpu.SemaphoreType.DMA((64,)),
        pltpu.SemaphoreType.DMA((64,)),
        pltpu.SemaphoreType.DMA((32,)),
        pltpu.SemaphoreType.DMA((2, 2)),
    ]
    ref_out, grad_gate, grad_up, g_text, g_image = pl.pallas_call(
        square_kernel,
        out_shape=outs,
        in_specs=[pl.BlockSpec(memory_space=pltpu.SMEM)] + [anywhere] * 13,
        out_specs=(anywhere,) * len(outs),
        scratch_shapes=scratch,
        compiler_params=pltpu.CompilerParams(
            collective_id=0, has_side_effects=True, vmem_limit_bytes=VMEM_BYTES
        ),
        name="square_step",
    )(
        pair_margin, ref_gate.T, ref_up.T, ref_residual, ref_modality.reshape(-1, LANES), ref_down_text.T, ref_down_image.T,
        pol_gate.T, pol_up.T, pol_modality.reshape(-1, LANES), pol_segment.reshape(-1, LANES), token_cotangent,
        pol_down_text.T, pol_down_image.T,
    )
    return (ref_out, grad_gate.T, grad_up.T, g_text.T, g_image.T)


def solution(mesh):
    n_fsdp, n_tp = mesh.shape["fsdp"], mesh.shape["tp"]
    two = P("fsdp", "tp")
    one = P("fsdp")
    in_specs = (two, two, two, one, two, two, two, two, one, one, P(), two, two, two)
    square = n_fsdp == 4 and n_tp == 2 * n_fsdp
    plan = square_per_device if square else per_device

    def body(*args):
        return plan(n_fsdp, n_tp, *args)

    return jax.shard_map(
        body, mesh=mesh, in_specs=in_specs, out_specs=(two,) * 5, check_vma=False
    )
```

```python
import jax
import jax.numpy as jnp
from jax import lax
from jax.experimental import pallas as pl
from jax.experimental.pallas import tpu as pltpu
from jax.sharding import PartitionSpec as P


MESH = pl.DeviceIdType.MESH
LANES = 128
VMEM_BYTES = 67043328

dpo_beta = 0.1


def silu_parts(gate, up):
    gate_f = gate.astype(jnp.float32)
    up_f = up.astype(jnp.float32)
    sig = jax.nn.sigmoid(gate_f)
    act = gate_f * sig
    return gate_f, up_f, sig, act


def hidden_of(gate, up):
    _, up_f, _, act = silu_parts(gate, up)
    return (act * up_f).astype(jnp.bfloat16)


def coef_of(pol_segment, pair_margin):
    seg_ids = jnp.arange(2 * pair_margin.shape[0], dtype=jnp.int32)
    pair_weight = dpo_beta * jax.nn.sigmoid(-dpo_beta * pair_margin)
    table = jnp.repeat(pair_weight, 2) * jnp.where(seg_ids % 2 == 0, -1.0, 1.0).astype(jnp.float32)
    return jnp.sum(
        jnp.where(pol_segment[:, None] == seg_ids[None, :], table[None, :], jnp.float32(0.0)),
        axis=1,
    )


def swap_pairs(n_fsdp, n_tp):
    r = n_tp // n_fsdp
    return [
        (f * n_tp + q * r + j, q * n_tp + f * r + j)
        for f in range(n_fsdp)
        for q in range(n_fsdp)
        for j in range(r)
    ]


def gather_modality(ref_modality, pol_modality, n_fsdp):
    own = jnp.stack([ref_modality, pol_modality])
    me = lax.axis_index("fsdp")
    both = jnp.zeros((n_fsdp,) + own.shape, own.dtype)
    both = lax.dynamic_update_index_in_dim(both, own, me, 0)
    for s in range(1, n_fsdp):
        got = lax.ppermute(own, "fsdp", [(i, (i + s) % n_fsdp) for i in range(n_fsdp)])
        both = lax.dynamic_update_index_in_dim(both, got, (me - s) % n_fsdp, 0)
    return both[:, 0].reshape(-1), both[:, 1].reshape(-1)


def per_device(
    n_fsdp,
    n_tp,
    ref_gate,
    ref_up,
    ref_residual,
    ref_modality,
    ref_down_text,
    ref_down_image,
    pol_gate,
    pol_up,
    pol_modality,
    pol_segment,
    pair_margin,
    token_cotangent,
    pol_down_text,
    pol_down_image,
):
    rows, feats = token_cotangent.shape
    pairs = swap_pairs(n_fsdp, n_tp)
    partner = [(t, t ^ 1) for t in range(n_tp)]
    index = lax.axis_index("tp")
    line, half = index // 2, index % 2

    def shift(step):
        return [(t, (t + 2 * step) % n_tp) for t in range(n_tp)]

    coef = coef_of(pol_segment, pair_margin)
    pol_own = hidden_of(pol_gate, pol_up)
    pol_hidden = lax.all_gather(pol_own, "fsdp", axis=0, tiled=True)
    ref_own = hidden_of(ref_gate, ref_up)
    ref_hidden = lax.all_gather(ref_own, "fsdp", axis=0, tiled=True)

    local_cot = (coef[:, None] * token_cotangent.astype(jnp.float32)).astype(jnp.bfloat16)
    moved = lax.ppermute(local_cot, ("fsdp", "tp"), pairs)
    modality_r, modality_p = gather_modality(ref_modality, pol_modality, n_fsdp)
    image_r = (modality_r == 1)[:, None]
    image_p = (modality_p == 1)[:, None]

    mine = jnp.zeros((n_fsdp, rows, feats), jnp.bfloat16)
    mine = lax.dynamic_update_index_in_dim(mine, moved, line, 0)
    for s in range(1, n_fsdp):
        got = lax.ppermute(moved, "tp", shift(s))
        mine = lax.dynamic_update_index_in_dim(mine, got, (line - s) % n_fsdp, 0)
    mine = mine.reshape(n_fsdp * rows, feats)
    theirs = lax.ppermute(mine, "tp", partner)
    first = half == 0
    cot_full = jnp.concatenate(
        [jnp.where(first, mine, theirs), jnp.where(first, theirs, mine)], axis=1
    )

    dh_text = jnp.dot(cot_full, pol_down_text, preferred_element_type=jnp.float32)
    dh_image = jnp.dot(cot_full, pol_down_image, preferred_element_type=jnp.float32)
    dh_part = jnp.where(image_p, dh_image, dh_text).astype(jnp.bfloat16)
    d_hidden = lax.psum_scatter(dh_part, "fsdp", scatter_dimension=0, tiled=True)

    zero = jnp.zeros_like(cot_full)
    over_rows = (((0,), (0,)), ((), ()))
    g_text = lax.dot_general(
        jnp.where(image_p, zero, cot_full), pol_hidden, over_rows, preferred_element_type=jnp.float32
    )
    g_image = lax.dot_general(
        jnp.where(image_p, cot_full, zero), pol_hidden, over_rows, preferred_element_type=jnp.float32
    )

    contract = (((1,), (1,)), ((), ()))

    def out_half(which):
        w_text = lax.dynamic_slice_in_dim(ref_down_text, which * feats, feats, 0)
        w_image = lax.dynamic_slice_in_dim(ref_down_image, which * feats, feats, 0)
        o_text = lax.dot_general(ref_hidden, w_text, contract, preferred_element_type=jnp.float32)
        o_image = lax.dot_general(ref_hidden, w_image, contract, preferred_element_type=jnp.float32)
        return jnp.where(image_r, o_image, o_text).astype(jnp.bfloat16)

    got = lax.ppermute(out_half(1 - half), "tp", partner)
    keep = out_half(half)
    both = (keep.astype(jnp.float32) + got.astype(jnp.float32)).astype(jnp.bfloat16)
    both = both.reshape(n_fsdp, rows, feats)
    total = lax.dynamic_index_in_dim(both, line, 0, keepdims=False).astype(jnp.float32)
    for s in range(1, n_fsdp):
        piece = lax.dynamic_index_in_dim(both, (line + s) % n_fsdp, 0, keepdims=False)
        total = total + lax.ppermute(piece, "tp", shift(s)).astype(jnp.float32)
    summed = lax.ppermute(total.astype(jnp.bfloat16), ("fsdp", "tp"), pairs)
    ref_out = (summed.astype(jnp.float32) + ref_residual.astype(jnp.float32)).astype(jnp.bfloat16)

    late_gate, late_up, d_hidden = lax.optimization_barrier((pol_gate, pol_up, d_hidden))
    gate_f, up_f, sig, act = silu_parts(late_gate, late_up)
    d_hidden = d_hidden.astype(jnp.float32)
    grad_gate = (d_hidden * up_f * sig * (1.0 + gate_f * (1.0 - sig))).astype(jnp.bfloat16)
    grad_up = (d_hidden * act).astype(jnp.bfloat16)
    return (ref_out, grad_gate, grad_up, g_text, g_image)


def square_kernel(
    margin, ref_gate, ref_up, residual, ref_mod, ref_text, ref_image, pol_gate, pol_up, pol_mod, pol_seg, cot_raw,
    pol_text, pol_image,
    out_o, own_o, got_o, early_x, late_x, early_y, late_y, gt_o, gi_o,
    href, hpv, tags, mod, own_cot, abuf, cot, w, sis_send, sis_recv, zs, zr, fin, rb, ra, dsend, drecv, gtile,
    ss, rs, ls, gs,
):
    n = cot.shape[1]
    rows, half = cot.shape[2], cot.shape[3]
    q = rows // n
    ff = href.shape[1]
    mid = ff // 2
    wide = 2 * LANES
    chunks = rows // wide
    f, t = lax.axis_index("fsdp"), lax.axis_index("tp")
    z, c = t // 2, t % 2
    oc = 1 - c
    fs = (f, f + 1 - 2 * (f % 2), (f + 2) % n, n - 1 - f)
    zp = [(z + r) % n for r in range(n)]
    zm = [(z + n - r) % n for r in range(n)]
    side = [(fs[s], t) for s in range(4)]
    up = [(f, 2 * zp[r] + c) for r in range(n)]
    sister = (f, 2 * z + oc)
    count = [0]
    lcount = [0]
    sends = []

    def remote(src, dst, dev):
        i = count[0]
        count[0] += 1
        copy = pltpu.make_async_remote_copy(
            src_ref=src, dst_ref=dst, send_sem=ss.at[i], recv_sem=rs.at[i],
            device_id=dev, device_id_type=MESH,
        )
        copy.start()
        sends.append(copy)
        return copy

    def local(src, dst):
        i = lcount[0]
        lcount[0] += 1
        copy = pltpu.make_async_copy(src, dst, ls.at[i])
        copy.start()
        return copy

    def piece(i):
        return pl.ds(pl.multiple_of(i * q, q), q)

    top, low = pl.ds(0, mid), pl.ds(mid, mid)
    loads = [
        [local(src.at[part], dsend.at[i, part]) for i, src in ((0, ref_gate), (1, ref_up))]
        for part in (top, low)
    ]
    small = [local(src, tags.at[i]) for i, src in enumerate((ref_mod, pol_mod, pol_seg))]
    small.append(local(cot_raw, own_cot))
    w_ld = [local(ref_text, w.at[0]), local(ref_image, w.at[1])]
    pol_ld = [local(pol_gate, dsend.at[2]), local(pol_up, dsend.at[3])]

    barrier = pltpu.get_barrier_semaphore()
    peers = [side[1], side[2], side[3]] + [up[r] for r in range(1, n)] + [sister]
    for peer in peers:
        pl.semaphore_signal(barrier, inc=1, device_id=peer, device_id_type=MESH)
    pl.semaphore_wait(barrier, len(peers))

    def hidden_rows(first, src, dst):
        @pl.loop(0, mid // 16)
        def _(i):
            at = pl.ds(pl.multiple_of(first + i * 16, 16), 16)
            gate = dsend[src, at, :].astype(jnp.float32)
            act = gate * jax.nn.sigmoid(gate)
            dst[0, at, :] = (act * dsend[src + 1, at, :].astype(jnp.float32)).astype(jnp.bfloat16)

    for copy in loads[0]:
        copy.wait()
    hidden_rows(0, 0, href)
    own_x = [remote(href.at[0, top], href.at[1, top], side[1])]
    for copy in loads[1]:
        copy.wait()
    hidden_rows(mid, 0, href)
    own_y = [remote(href.at[0, low], href.at[2, low], side[2])]
    for copy in small:
        copy.wait()

    def tag_row(i, size):
        return jnp.concatenate(
            [jnp.broadcast_to(tags[i, j : j + 1, :], (size, LANES)) for j in range(rows // LANES)], axis=1
        )

    seg = tag_row(2, 8)
    coef = jnp.zeros((8, rows), jnp.float32)
    for p in range(margin.shape[0]):
        weight = dpo_beta * jax.nn.sigmoid(-dpo_beta * jnp.full((8, rows), margin[p], jnp.float32))
        coef = jnp.where(seg // 2 == p, weight, coef)
    coef = jnp.where(seg % 2 == 0, -coef, coef).T[:, 0:1]
    own_cot[...] = (coef * own_cot[...].astype(jnp.float32)).astype(jnp.bfloat16)
    row = lax.broadcasted_iota(jnp.int32, (16, rows), 0)
    both = jnp.where(row == 0, tag_row(0, 16), jnp.where(row == 1, tag_row(1, 16), 0))
    mod[0] = both.astype(jnp.float32).astype(jnp.bfloat16)
    a_cp = [remote(own_cot.at[piece(zp[r])], abuf.at[z], up[r]) for r in range(1, n)]
    m_cp = [remote(mod.at[0], mod.at[s], side[s]) for s in range(1, 4)]
    abuf[z] = own_cot[piece(z), :]
    for copy in pol_ld:
        copy.wait()
    hidden_rows(0, 2, hpv)
    hidden_rows(mid, 2, hpv)

    for copy in a_cp:
        copy.wait_recv()
    b_cp = [remote(abuf.at[fs[s]], cot.at[c, s, piece(z)], side[s]) for s in range(1, 4)]
    own_x.append(remote(href.at[0, low], href.at[1, low], side[1]))
    own_y.append(remote(href.at[0, top], href.at[2, top], side[2]))
    cot[c, 0, piece(z), :] = abuf[f]

    def lanes(j, size):
        return pl.ds(pl.multiple_of(j * size, size), size)

    over_ff = (((0,), (0,)), ((), ()))

    def out_rows(s, j, which):
        cols = lanes(which, half)
        image = mod[s, :, lanes(j, wide)][0:1]
        h = href[s, :, lanes(j, wide)]
        h_image = h * image
        h_text = h * (1.0 - image)
        o_text = lax.dot_general(h_text, w[0, :, cols], over_ff, preferred_element_type=jnp.float32)
        o_image = lax.dot_general(h_image, w[1, :, cols], over_ff, preferred_element_type=jnp.float32)
        return o_text + o_image

    e_cp = {}
    f_cp = []

    def out_other(s):
        @pl.loop(0, chunks)
        def _(j):
            sis_send[s, lanes(j, wide), :] = out_rows(s, j, oc).astype(jnp.bfloat16)

        e_cp[s] = remote(sis_send.at[s], sis_recv.at[s], sister)

    def out_own(s):
        e_cp[s].wait_recv()

        @pl.loop(0, chunks)
        def _(j):
            total = out_rows(s, j, c) + sis_recv[s, lanes(j, wide), :].astype(jnp.float32)
            zs[s, lanes(j, wide), :] = total.astype(jnp.bfloat16)

        for r in range(1, n):
            f_cp.append(remote(zs.at[s, piece(zp[r])], zr.at[r - 1, s], up[r]))

    for copy in w_ld:
        copy.wait()
    out_other(0)
    for copy in b_cp:
        copy.wait_recv()
    c_cp = [remote(cot.at[c, :, piece(z)], cot.at[c, :, piece(z)], up[r]) for r in range(1, n)]
    d_cp = [remote(cot.at[c, :, piece(z)], cot.at[c, :, piece(z)], sister)]
    own_x[0].wait_recv()
    fwd_y = remote(href.at[1, top], href.at[3, top], side[2])
    own_y[0].wait_recv()
    fwd_x = remote(href.at[2, low], href.at[3, low], side[1])
    out_own(0)
    pol_x = [remote(hpv.at[0, part], hpv.at[1, part], side[1]) for part in (top, low)]
    pol_y = [remote(hpv.at[0, part], hpv.at[2, part], side[2]) for part in (low, top)]
    for copy in m_cp:
        copy.wait_recv()
    own_x[1].wait_recv()
    own_y[1].wait_recv()
    out_other(1)
    out_other(2)
    out_own(1)
    out_own(2)
    fwd_y.wait_recv()
    fwd_x.wait_recv()
    out_other(3)
    out_own(3)
    pol_x[0].wait_recv()
    polf_y = remote(hpv.at[1, top], hpv.at[3, top], side[2])
    pol_y[0].wait_recv()
    polf_x = remote(hpv.at[2, low], hpv.at[3, low], side[1])
    for r in range(1, n):
        c_cp[r - 1].wait_recv()
        d_cp.append(remote(cot.at[c, :, piece(zm[r])], cot.at[c, :, piece(zm[r])], sister))
    w_ld = [local(pol_text, w.at[0]), local(pol_image, w.at[1])]
    for copy in d_cp:
        copy.wait_recv()
    for copy in w_ld:
        copy.wait()
    for copy in a_cp:
        copy.wait_send()
    res_ld = local(residual, own_cot)

    over_last = (((1,), (1,)), ((), ()))

    def dh_part(s, first, got):
        part = pl.ds(first, mid)

        @pl.loop(0, chunks)
        def _(j):
            at = lanes(j, wide)

            def of(i):
                lo = lax.dot_general(
                    w[i, part, :half], cot[0, s, at, :], over_last, preferred_element_type=jnp.float32
                )
                return lo + lax.dot_general(
                    w[i, part, half:], cot[1, s, at, :], over_last, preferred_element_type=jnp.float32
                )

            row = mod[s, :, at].astype(jnp.float32)[1:2]
            image = jnp.broadcast_to(row, (mid, wide)) > 0.5
            d = jnp.where(image, of(1), of(0))
            if got is not None:
                d = d + drecv[got, :, at].astype(jnp.float32)
            dsend[s, part, at] = d.astype(jnp.bfloat16)

    dh_part(3, 0, None)
    i_x = remote(dsend.at[3, top], drecv.at[0], side[1])
    dh_part(3, mid, None)
    i_y = remote(dsend.at[3, low], drecv.at[1], side[2])
    dh_part(1, 0, None)
    dh_part(2, mid, None)
    dh_part(0, 0, None)
    dh_part(0, mid, None)
    done = [local(dsend.at[0], own_o)]

    for copy in [pol_x[1], pol_y[1], polf_x, polf_y]:
        copy.wait_recv()
    per_half = half // wide
    tiles = 2 * per_half

    def g_copies(i):
        slot, a, j = i % 2, i // tiles, i % tiles
        at = pl.ds(pl.multiple_of(a * mid, mid), mid)
        return (
            pltpu.make_async_copy(gtile.at[slot, 0], gt_o.at[at, lanes(j, wide)], gs.at[slot, 0]),
            pltpu.make_async_copy(gtile.at[slot, 1], gi_o.at[at, lanes(j, wide)], gs.at[slot, 1]),
        )

    def g_tile(i):
        a, j = i // tiles, i % tiles
        at = pl.ds(pl.multiple_of(a * mid, mid), mid)
        g_text, g_image = None, None
        for s in range(4):
            y = cot[j // per_half, s, :, lanes(j % per_half, wide)]
            image = mod[s][1:2]
            h = hpv[s, at, :]
            t_text = jnp.dot(h * (1.0 - image), y, preferred_element_type=jnp.float32)
            t_image = jnp.dot(h * image, y, preferred_element_type=jnp.float32)
            g_text = t_text if g_text is None else g_text + t_text
            g_image = t_image if g_image is None else g_image + t_image

        @pl.when(i >= 2)
        def _():
            for copy in g_copies(i - 2):
                copy.wait()

        gtile[i % 2, 0] = g_text
        gtile[i % 2, 1] = g_image
        for copy in g_copies(i):
            copy.start()

    pl.loop(0, tiles)(g_tile)

    for copy in f_cp:
        copy.wait_recv()
    for s in range(4):
        total = zs[s, piece(z), :].astype(jnp.float32)
        for r in range(1, n):
            total = total + zr[r - 1, s].astype(jnp.float32)
        fin[s] = total.astype(jnp.bfloat16)
    rb[f] = fin[0]
    g_cp = [remote(fin.at[s], rb.at[f], side[s]) for s in range(1, 4)]
    j_cp = [
        remote(dsend.at[1, top], got_o.at[top], side[1]),
        remote(dsend.at[2, low], got_o.at[low], side[2]),
    ]
    i_y.wait_recv()
    dh_part(1, mid, 1)
    fore, aft = pl.ds(0, early_x.shape[1]), pl.ds(early_x.shape[1], late_x.shape[1])
    done += [local(dsend.at[1, low, fore], early_x), local(dsend.at[1, low, aft], late_x)]
    i_x.wait_recv()
    dh_part(2, 0, 0)
    done += [local(dsend.at[2, top, fore], early_y), local(dsend.at[2, top, aft], late_y)]
    for copy in g_cp:
        copy.wait_recv()
    h_cp = [remote(rb.at[zp[r]], ra.at[z], up[r]) for r in range(1, n)]
    ra[z] = rb[z]
    pl.loop(tiles, 2 * tiles)(g_tile)
    res_ld.wait()
    for copy in h_cp:
        copy.wait_recv()
    total = own_cot[...].astype(jnp.float32) + ra[...].reshape(rows, half).astype(jnp.float32)
    own_cot[...] = total.astype(jnp.bfloat16)
    done.append(local(own_cot, out_o))
    for i in (2 * tiles - 2, 2 * tiles - 1):
        for copy in g_copies(i):
            copy.wait()
    for copy in done:
        copy.wait()
    for copy in j_cp:
        copy.wait_recv()
    for copy in sends:
        if all(copy is not other for other in a_cp):
            copy.wait_send()


def write_kernel(out, g_text, g_image, out_o, gt_o, gi_o):
    out_o[...] = out[...]
    gt_o[...] = g_text[...]
    gi_o[...] = g_image[...]


def grad_kernel(own, got, last_x, last_y, gate, up, *refs):
    gg_o, gu_o = refs[-2:]
    height, count = own.shape[0], 16

    def rows_of(last):
        for i in range(height // count):
            at = pl.ds(i * count, count)
            d = own[at, :].astype(jnp.float32) + got[at, :].astype(jnp.float32) + last[at, :].astype(jnp.float32)
            gate_f, up_f, sig, act = silu_parts(gate[at, :], up[at, :])
            gg_o[at, :] = (d * up_f * sig * (1.0 + gate_f * (1.0 - sig))).astype(jnp.bfloat16)
            gu_o[at, :] = (d * act).astype(jnp.bfloat16)

    @pl.when(pl.program_id(0) == 0)
    def _():
        rows_of(last_y)

    @pl.when(pl.program_id(0) == 1)
    def _():
        rows_of(last_x)


def grad_call(own, got, last_x, last_y, gate, up, skip, so_far):
    ff, rows = own.shape
    wide = 2 * LANES
    steps = last_x.shape[1] // wide
    tile = (ff // 2, wide)
    every = pl.BlockSpec(tile, lambda a, j: (a, j + skip))
    anywhere = pl.BlockSpec(memory_space=pl.ANY)
    cells = 2 * last_x.shape[0] * last_x.shape[1]
    block = jax.ShapeDtypeStruct((ff, rows), jnp.bfloat16)
    return pl.pallas_call(
        grad_kernel,
        grid=(2, steps),
        out_shape=(block, block),
        in_specs=[
            every,
            every,
            pl.BlockSpec(tile, lambda a, j: (0, a * j)),
            pl.BlockSpec(tile, lambda a, j: (0, (1 - a) * j + a * (steps - 1))),
            every,
            every,
        ]
        + [anywhere] * len(so_far),
        out_specs=(every, every),
        input_output_aliases={6 + i: i for i in range(len(so_far))},
        compiler_params=pltpu.CompilerParams(
            dimension_semantics=("arbitrary", "arbitrary"), vmem_limit_bytes=VMEM_BYTES
        ),
        cost_estimate=pl.CostEstimate(flops=1000 * cells, bytes_accessed=14 * cells, transcendentals=cells),
        name="gate_grads",
    )(own, got, last_x, last_y, gate, up, *so_far)


def square_per_device(
    n_fsdp,
    n_tp,
    ref_gate,
    ref_up,
    ref_residual,
    ref_modality,
    ref_down_text,
    ref_down_image,
    pol_gate,
    pol_up,
    pol_modality,
    pol_segment,
    pair_margin,
    token_cotangent,
    pol_down_text,
    pol_down_image,
):
    rows, feats = token_cotangent.shape
    ff = ref_gate.shape[1]
    n = n_fsdp
    q = rows // n
    bf16 = jnp.bfloat16
    shape = jax.ShapeDtypeStruct
    block = shape((ff, rows), bf16)
    grad = shape((ff, 2 * feats), jnp.float32)
    anywhere = pl.BlockSpec(memory_space=pl.ANY)
    aft = rows // (3 * LANES) * LANES
    fore_part, aft_part = shape((ff // 2, rows - aft), bf16), shape((ff // 2, aft), bf16)
    outs = (
        shape((rows, feats), bf16), block, block, fore_part, aft_part, fore_part, aft_part, grad, grad,
    )
    scratch = [
        pltpu.VMEM((4, ff, rows), bf16),
        pltpu.VMEM((4, ff, rows), bf16),
        pltpu.VMEM((3, rows // LANES, LANES), jnp.int32),
        pltpu.VMEM((4, 16, rows), bf16),
        pltpu.VMEM((rows, feats), bf16),
        pltpu.VMEM((n, q, feats), bf16),
        pltpu.VMEM((2, 4, rows, feats), bf16),
        pltpu.VMEM((2, ff, 2 * feats), bf16),
        pltpu.VMEM((4, rows, feats), bf16),
        pltpu.VMEM((4, rows, feats), bf16),
        pltpu.VMEM((4, rows, feats), bf16),
        pltpu.VMEM((n - 1, 4, q, feats), bf16),
        pltpu.VMEM((4, q, feats), bf16),
        pltpu.VMEM((4, q, feats), bf16),
        pltpu.VMEM((4, q, feats), bf16),
        pltpu.VMEM((4, ff, rows), bf16),
        pltpu.VMEM((2, ff // 2, rows), bf16),
        pltpu.VMEM((2, 2, ff // 2, 2 * LANES), jnp.float32),
        pltpu.SemaphoreType.DMA((64,)),
        pltpu.SemaphoreType.DMA((64,)),
        pltpu.SemaphoreType.DMA((32,)),
        pltpu.SemaphoreType.DMA((2, 2)),
    ]
    out, own, got, early_x, late_x, early_y, late_y, g_text, g_image = pl.pallas_call(
        square_kernel,
        out_shape=outs,
        in_specs=[pl.BlockSpec(memory_space=pltpu.SMEM)] + [anywhere] * 13,
        out_specs=(anywhere,) * len(outs),
        scratch_shapes=scratch,
        compiler_params=pltpu.CompilerParams(
            collective_id=0, has_side_effects=True, vmem_limit_bytes=VMEM_BYTES
        ),
        name="square_step",
    )(
        pair_margin, ref_gate.T, ref_up.T, ref_residual, ref_modality.reshape(-1, LANES), ref_down_text.T, ref_down_image.T,
        pol_gate.T, pol_up.T, pol_modality.reshape(-1, LANES), pol_segment.reshape(-1, LANES), token_cotangent,
        pol_down_text.T, pol_down_image.T,
    )
    across_x = [(i, i + 1 - 2 * (i % 2)) for i in range(n)]
    across_y = [(i, (i + 2) % n) for i in range(n)]
    early_x = lax.ppermute(early_x, "fsdp", across_x)
    early_y = lax.ppermute(early_y, "fsdp", across_y)
    late_x = lax.ppermute(late_x, "fsdp", across_x)
    late_y = lax.ppermute(late_y, "fsdp", across_y)

    wide = 2 * LANES
    steps = 2 * feats // wide
    out_spec = pl.BlockSpec((rows // (2 * steps), feats), lambda a, j: (a * steps + j, 0))
    g_spec = pl.BlockSpec((ff // 2, wide), lambda a, j: (a, j))
    ref_out, g_text, g_image = pl.pallas_call(
        write_kernel,
        grid=(2, steps),
        out_shape=(shape((rows, feats), bf16), grad, grad),
        in_specs=[out_spec, g_spec, g_spec],
        out_specs=(out_spec, g_spec, g_spec),
        compiler_params=pltpu.CompilerParams(
            dimension_semantics=("arbitrary", "arbitrary"), vmem_limit_bytes=VMEM_BYTES
        ),
        cost_estimate=pl.CostEstimate(
            flops=1000 * ff * feats, bytes_accessed=32 * ff * feats, transcendentals=0
        ),
        name="write_out",
    )(out, g_text, g_image)

    grads = grad_call(own, got, early_x, early_y, pol_gate.T, pol_up.T, 0, ())
    skip = (rows - aft) // (2 * LANES)
    grad_gate, grad_up = grad_call(own, got, late_x, late_y, pol_gate.T, pol_up.T, skip, grads)
    return (ref_out, grad_gate.T, grad_up.T, g_text.T, g_image.T)


def solution(mesh):
    n_fsdp, n_tp = mesh.shape["fsdp"], mesh.shape["tp"]
    two = P("fsdp", "tp")
    one = P("fsdp")
    in_specs = (two, two, two, one, two, two, two, two, one, one, P(), two, two, two)
    square = n_fsdp == 4 and n_tp == 2 * n_fsdp
    plan = square_per_device if square else per_device

    def body(*args):
        return plan(n_fsdp, n_tp, *args)

    return jax.shard_map(
        body, mesh=mesh, in_specs=in_specs, out_specs=(two,) * 5, check_vma=False
    )
```

```python
import jax
import jax.numpy as jnp
from jax import lax
from jax.experimental import pallas as pl
from jax.experimental.pallas import tpu as pltpu
from jax.sharding import PartitionSpec as P


MESH = pl.DeviceIdType.MESH
LANES = 128
VMEM_BYTES = 67043328

dpo_beta = 0.1


def silu_parts(gate, up):
    gate_f = gate.astype(jnp.float32)
    up_f = up.astype(jnp.float32)
    sig = jax.nn.sigmoid(gate_f)
    act = gate_f * sig
    return gate_f, up_f, sig, act


def hidden_of(gate, up):
    _, up_f, _, act = silu_parts(gate, up)
    return (act * up_f).astype(jnp.bfloat16)


def coef_of(pol_segment, pair_margin):
    seg_ids = jnp.arange(2 * pair_margin.shape[0], dtype=jnp.int32)
    pair_weight = dpo_beta * jax.nn.sigmoid(-dpo_beta * pair_margin)
    table = jnp.repeat(pair_weight, 2) * jnp.where(seg_ids % 2 == 0, -1.0, 1.0).astype(jnp.float32)
    return jnp.sum(
        jnp.where(pol_segment[:, None] == seg_ids[None, :], table[None, :], jnp.float32(0.0)),
        axis=1,
    )


def swap_pairs(n_fsdp, n_tp):
    r = n_tp // n_fsdp
    return [
        (f * n_tp + q * r + j, q * n_tp + f * r + j)
        for f in range(n_fsdp)
        for q in range(n_fsdp)
        for j in range(r)
    ]


def gather_modality(ref_modality, pol_modality, n_fsdp):
    own = jnp.stack([ref_modality, pol_modality])
    me = lax.axis_index("fsdp")
    both = jnp.zeros((n_fsdp,) + own.shape, own.dtype)
    both = lax.dynamic_update_index_in_dim(both, own, me, 0)
    for s in range(1, n_fsdp):
        got = lax.ppermute(own, "fsdp", [(i, (i + s) % n_fsdp) for i in range(n_fsdp)])
        both = lax.dynamic_update_index_in_dim(both, got, (me - s) % n_fsdp, 0)
    return both[:, 0].reshape(-1), both[:, 1].reshape(-1)


def per_device(
    n_fsdp,
    n_tp,
    ref_gate,
    ref_up,
    ref_residual,
    ref_modality,
    ref_down_text,
    ref_down_image,
    pol_gate,
    pol_up,
    pol_modality,
    pol_segment,
    pair_margin,
    token_cotangent,
    pol_down_text,
    pol_down_image,
):
    rows, feats = token_cotangent.shape
    pairs = swap_pairs(n_fsdp, n_tp)
    partner = [(t, t ^ 1) for t in range(n_tp)]
    index = lax.axis_index("tp")
    line, half = index // 2, index % 2

    def shift(step):
        return [(t, (t + 2 * step) % n_tp) for t in range(n_tp)]

    coef = coef_of(pol_segment, pair_margin)
    pol_own = hidden_of(pol_gate, pol_up)
    pol_hidden = lax.all_gather(pol_own, "fsdp", axis=0, tiled=True)
    ref_own = hidden_of(ref_gate, ref_up)
    ref_hidden = lax.all_gather(ref_own, "fsdp", axis=0, tiled=True)

    local_cot = (coef[:, None] * token_cotangent.astype(jnp.float32)).astype(jnp.bfloat16)
    moved = lax.ppermute(local_cot, ("fsdp", "tp"), pairs)
    modality_r, modality_p = gather_modality(ref_modality, pol_modality, n_fsdp)
    image_r = (modality_r == 1)[:, None]
    image_p = (modality_p == 1)[:, None]

    mine = jnp.zeros((n_fsdp, rows, feats), jnp.bfloat16)
    mine = lax.dynamic_update_index_in_dim(mine, moved, line, 0)
    for s in range(1, n_fsdp):
        got = lax.ppermute(moved, "tp", shift(s))
        mine = lax.dynamic_update_index_in_dim(mine, got, (line - s) % n_fsdp, 0)
    mine = mine.reshape(n_fsdp * rows, feats)
    theirs = lax.ppermute(mine, "tp", partner)
    first = half == 0
    cot_full = jnp.concatenate(
        [jnp.where(first, mine, theirs), jnp.where(first, theirs, mine)], axis=1
    )

    dh_text = jnp.dot(cot_full, pol_down_text, preferred_element_type=jnp.float32)
    dh_image = jnp.dot(cot_full, pol_down_image, preferred_element_type=jnp.float32)
    dh_part = jnp.where(image_p, dh_image, dh_text).astype(jnp.bfloat16)
    d_hidden = lax.psum_scatter(dh_part, "fsdp", scatter_dimension=0, tiled=True)

    zero = jnp.zeros_like(cot_full)
    over_rows = (((0,), (0,)), ((), ()))
    g_text = lax.dot_general(
        jnp.where(image_p, zero, cot_full), pol_hidden, over_rows, preferred_element_type=jnp.float32
    )
    g_image = lax.dot_general(
        jnp.where(image_p, cot_full, zero), pol_hidden, over_rows, preferred_element_type=jnp.float32
    )

    contract = (((1,), (1,)), ((), ()))

    def out_half(which):
        w_text = lax.dynamic_slice_in_dim(ref_down_text, which * feats, feats, 0)
        w_image = lax.dynamic_slice_in_dim(ref_down_image, which * feats, feats, 0)
        o_text = lax.dot_general(ref_hidden, w_text, contract, preferred_element_type=jnp.float32)
        o_image = lax.dot_general(ref_hidden, w_image, contract, preferred_element_type=jnp.float32)
        return jnp.where(image_r, o_image, o_text).astype(jnp.bfloat16)

    got = lax.ppermute(out_half(1 - half), "tp", partner)
    keep = out_half(half)
    both = (keep.astype(jnp.float32) + got.astype(jnp.float32)).astype(jnp.bfloat16)
    both = both.reshape(n_fsdp, rows, feats)
    total = lax.dynamic_index_in_dim(both, line, 0, keepdims=False).astype(jnp.float32)
    for s in range(1, n_fsdp):
        piece = lax.dynamic_index_in_dim(both, (line + s) % n_fsdp, 0, keepdims=False)
        total = total + lax.ppermute(piece, "tp", shift(s)).astype(jnp.float32)
    summed = lax.ppermute(total.astype(jnp.bfloat16), ("fsdp", "tp"), pairs)
    ref_out = (summed.astype(jnp.float32) + ref_residual.astype(jnp.float32)).astype(jnp.bfloat16)

    late_gate, late_up, d_hidden = lax.optimization_barrier((pol_gate, pol_up, d_hidden))
    gate_f, up_f, sig, act = silu_parts(late_gate, late_up)
    d_hidden = d_hidden.astype(jnp.float32)
    grad_gate = (d_hidden * up_f * sig * (1.0 + gate_f * (1.0 - sig))).astype(jnp.bfloat16)
    grad_up = (d_hidden * act).astype(jnp.bfloat16)
    return (ref_out, grad_gate, grad_up, g_text, g_image)


def square_kernel(
    margin, ref_gate, ref_up, residual, ref_mod, ref_text, ref_image, pol_gate, pol_up, pol_mod, pol_seg, cot_raw,
    pol_text, pol_image,
    out_o, own_o, got_o, early_x, late_x, early_y, late_y, gt_o, gi_o,
    href, hpv, tags, mod, own_cot, abuf, cot, w, sis_send, sis_recv, zs, zr, fin, rb, ra, dsend, drecv, gtile,
    ss, rs, ls, gs,
):
    n = cot.shape[1]
    rows, half = cot.shape[2], cot.shape[3]
    q = rows // n
    ff = href.shape[1]
    mid = ff // 2
    wide = 2 * LANES
    chunks = rows // wide
    f, t = lax.axis_index("fsdp"), lax.axis_index("tp")
    z, c = t // 2, t % 2
    oc = 1 - c
    fs = (f, f + 1 - 2 * (f % 2), (f + 2) % n, n - 1 - f)
    zp = [(z + r) % n for r in range(n)]
    zm = [(z + n - r) % n for r in range(n)]
    side = [(fs[s], t) for s in range(4)]
    up = [(f, 2 * zp[r] + c) for r in range(n)]
    sister = (f, 2 * z + oc)
    count = [0]
    lcount = [0]
    sends = []

    def remote(src, dst, dev):
        i = count[0]
        count[0] += 1
        copy = pltpu.make_async_remote_copy(
            src_ref=src, dst_ref=dst, send_sem=ss.at[i], recv_sem=rs.at[i],
            device_id=dev, device_id_type=MESH,
        )
        copy.start()
        sends.append(copy)
        return copy

    def local(src, dst):
        i = lcount[0]
        lcount[0] += 1
        copy = pltpu.make_async_copy(src, dst, ls.at[i])
        copy.start()
        return copy

    def piece(i):
        return pl.ds(pl.multiple_of(i * q, q), q)

    top, low = pl.ds(0, mid), pl.ds(mid, mid)
    loads = [
        [local(src.at[part], dsend.at[i, part]) for i, src in ((0, ref_gate), (1, ref_up))]
        for part in (top, low)
    ]
    small = [local(src, tags.at[i]) for i, src in enumerate((ref_mod, pol_mod, pol_seg))]
    small.append(local(cot_raw, own_cot))

    barrier = pltpu.get_barrier_semaphore()
    peers = [side[1], side[2], side[3]] + [up[r] for r in range(1, n)] + [sister]
    for peer in peers:
        pl.semaphore_signal(barrier, inc=1, device_id=peer, device_id_type=MESH)
    pl.semaphore_wait(barrier, len(peers))

    def hidden_rows(first, src, dst):
        @pl.loop(0, mid // 16)
        def _(i):
            at = pl.ds(pl.multiple_of(first + i * 16, 16), 16)
            gate = dsend[src, at, :].astype(jnp.float32)
            act = gate * jax.nn.sigmoid(gate)
            dst[0, at, :] = (act * dsend[src + 1, at, :].astype(jnp.float32)).astype(jnp.bfloat16)

    for copy in loads[0]:
        copy.wait()
    hidden_rows(0, 0, href)
    own_x = [remote(href.at[0, top], href.at[1, top], side[1])]
    pol_ld = [local(pol_gate, dsend.at[2]), local(pol_up, dsend.at[3])]
    w_ld = [local(ref_text, w.at[0]), local(ref_image, w.at[1])]
    for copy in loads[1]:
        copy.wait()
    hidden_rows(mid, 0, href)
    own_y = [remote(href.at[0, low], href.at[2, low], side[2])]
    for copy in small:
        copy.wait()

    def tag_row(i, size):
        return jnp.concatenate(
            [jnp.broadcast_to(tags[i, j : j + 1, :], (size, LANES)) for j in range(rows // LANES)], axis=1
        )

    seg = tag_row(2, 8)
    coef = jnp.zeros((8, rows), jnp.float32)
    for p in range(margin.shape[0]):
        weight = dpo_beta * jax.nn.sigmoid(-dpo_beta * jnp.full((8, rows), margin[p], jnp.float32))
        coef = jnp.where(seg // 2 == p, weight, coef)
    coef = jnp.where(seg % 2 == 0, -coef, coef).T[:, 0:1]
    own_cot[...] = (coef * own_cot[...].astype(jnp.float32)).astype(jnp.bfloat16)
    row = lax.broadcasted_iota(jnp.int32, (16, rows), 0)
    both = jnp.where(row == 0, tag_row(0, 16), jnp.where(row == 1, tag_row(1, 16), 0))
    mod[0] = both.astype(jnp.float32).astype(jnp.bfloat16)
    a_cp = [remote(own_cot.at[piece(zp[r])], abuf.at[z], up[r]) for r in range(1, n)]
    m_cp = [remote(mod.at[0], mod.at[s], side[s]) for s in range(1, 4)]
    abuf[z] = own_cot[piece(z), :]
    for copy in pol_ld:
        copy.wait()
    hidden_rows(0, 2, hpv)
    hidden_rows(mid, 2, hpv)

    for copy in a_cp:
        copy.wait_recv()
    b_cp = [remote(abuf.at[fs[s]], cot.at[c, s, piece(z)], side[s]) for s in range(1, 4)]
    own_x.append(remote(href.at[0, low], href.at[1, low], side[1]))
    own_y.append(remote(href.at[0, top], href.at[2, top], side[2]))
    cot[c, 0, piece(z), :] = abuf[f]

    def lanes(j, size):
        return pl.ds(pl.multiple_of(j * size, size), size)

    over_ff = (((0,), (0,)), ((), ()))

    def out_rows(s, j, which):
        cols = lanes(which, half)
        image = mod[s, :, lanes(j, wide)][0:1]
        h = href[s, :, lanes(j, wide)]
        h_image = h * image
        h_text = h * (1.0 - image)
        o_text = lax.dot_general(h_text, w[0, :, cols], over_ff, preferred_element_type=jnp.float32)
        o_image = lax.dot_general(h_image, w[1, :, cols], over_ff, preferred_element_type=jnp.float32)
        return o_text + o_image

    e_cp = {}
    f_cp = []

    def out_other(s):
        @pl.loop(0, chunks)
        def _(j):
            sis_send[s, lanes(j, wide), :] = out_rows(s, j, oc).astype(jnp.bfloat16)

        e_cp[s] = remote(sis_send.at[s], sis_recv.at[s], sister)

    def out_own(s):
        e_cp[s].wait_recv()

        @pl.loop(0, chunks)
        def _(j):
            total = out_rows(s, j, c) + sis_recv[s, lanes(j, wide), :].astype(jnp.float32)
            zs[s, lanes(j, wide), :] = total.astype(jnp.bfloat16)

        for r in range(1, n):
            f_cp.append(remote(zs.at[s, piece(zp[r])], zr.at[r - 1, s], up[r]))

    for copy in w_ld:
        copy.wait()
    out_other(0)
    for copy in b_cp:
        copy.wait_recv()
    c_cp = [remote(cot.at[c, :, piece(z)], cot.at[c, :, piece(z)], up[r]) for r in range(1, n)]
    d_cp = [remote(cot.at[c, :, piece(z)], cot.at[c, :, piece(z)], sister)]
    own_x[0].wait_recv()
    fwd_y = remote(href.at[1, top], href.at[3, top], side[2])
    own_y[0].wait_recv()
    fwd_x = remote(href.at[2, low], href.at[3, low], side[1])
    out_own(0)
    pol_x = [remote(hpv.at[0, part], hpv.at[1, part], side[1]) for part in (top, low)]
    pol_y = [remote(hpv.at[0, part], hpv.at[2, part], side[2]) for part in (low, top)]
    for copy in m_cp:
        copy.wait_recv()
    own_x[1].wait_recv()
    own_y[1].wait_recv()
    out_other(1)
    out_other(2)
    out_own(1)
    out_own(2)
    fwd_y.wait_recv()
    fwd_x.wait_recv()
    out_other(3)
    out_own(3)
    pol_x[0].wait_recv()
    polf_y = remote(hpv.at[1, top], hpv.at[3, top], side[2])
    pol_y[0].wait_recv()
    polf_x = remote(hpv.at[2, low], hpv.at[3, low], side[1])
    for r in range(1, n):
        c_cp[r - 1].wait_recv()
        d_cp.append(remote(cot.at[c, :, piece(zm[r])], cot.at[c, :, piece(zm[r])], sister))
    w_ld = [local(pol_text, w.at[0]), local(pol_image, w.at[1])]
    for copy in d_cp:
        copy.wait_recv()
    for copy in w_ld:
        copy.wait()
    for copy in a_cp:
        copy.wait_send()
    res_ld = local(residual, own_cot)

    over_last = (((1,), (1,)), ((), ()))

    def dh_part(s, first, got):
        part = pl.ds(first, mid)

        @pl.loop(0, chunks)
        def _(j):
            at = lanes(j, wide)

            def of(i):
                lo = lax.dot_general(
                    w[i, part, :half], cot[0, s, at, :], over_last, preferred_element_type=jnp.float32
                )
                return lo + lax.dot_general(
                    w[i, part, half:], cot[1, s, at, :], over_last, preferred_element_type=jnp.float32
                )

            row = mod[s, :, at].astype(jnp.float32)[1:2]
            image = jnp.broadcast_to(row, (mid, wide)) > 0.5
            d = jnp.where(image, of(1), of(0))
            if got is not None:
                d = d + drecv[got, :, at].astype(jnp.float32)
            dsend[s, part, at] = d.astype(jnp.bfloat16)

    dh_part(3, 0, None)
    i_x = remote(dsend.at[3, top], drecv.at[0], side[1])
    dh_part(3, mid, None)
    i_y = remote(dsend.at[3, low], drecv.at[1], side[2])
    dh_part(1, 0, None)
    dh_part(2, mid, None)
    dh_part(0, 0, None)
    dh_part(0, mid, None)
    done = [local(dsend.at[0], own_o)]

    for copy in [pol_x[1], pol_y[1], polf_x, polf_y]:
        copy.wait_recv()
    per_half = half // wide
    tiles = 2 * per_half

    def g_copies(i):
        slot, a, j = i % 2, i // tiles, i % tiles
        at = pl.ds(pl.multiple_of(a * mid, mid), mid)
        return (
            pltpu.make_async_copy(gtile.at[slot, 0], gt_o.at[at, lanes(j, wide)], gs.at[slot, 0]),
            pltpu.make_async_copy(gtile.at[slot, 1], gi_o.at[at, lanes(j, wide)], gs.at[slot, 1]),
        )

    def g_tile(i):
        a, j = i // tiles, i % tiles
        at = pl.ds(pl.multiple_of(a * mid, mid), mid)
        g_text, g_image = None, None
        for s in range(4):
            y = cot[j // per_half, s, :, lanes(j % per_half, wide)]
            image = mod[s][1:2]
            h = hpv[s, at, :]
            t_text = jnp.dot(h * (1.0 - image), y, preferred_element_type=jnp.float32)
            t_image = jnp.dot(h * image, y, preferred_element_type=jnp.float32)
            g_text = t_text if g_text is None else g_text + t_text
            g_image = t_image if g_image is None else g_image + t_image

        @pl.when(i >= 2)
        def _():
            for copy in g_copies(i - 2):
                copy.wait()

        gtile[i % 2, 0] = g_text
        gtile[i % 2, 1] = g_image
        for copy in g_copies(i):
            copy.start()

    pl.loop(0, tiles)(g_tile)

    for copy in f_cp:
        copy.wait_recv()
    for s in range(4):
        total = zs[s, piece(z), :].astype(jnp.float32)
        for r in range(1, n):
            total = total + zr[r - 1, s].astype(jnp.float32)
        fin[s] = total.astype(jnp.bfloat16)
    rb[f] = fin[0]
    g_cp = [remote(fin.at[s], rb.at[f], side[s]) for s in range(1, 4)]
    j_cp = [
        remote(dsend.at[1, top], got_o.at[top], side[1]),
        remote(dsend.at[2, low], got_o.at[low], side[2]),
    ]
    i_y.wait_recv()
    dh_part(1, mid, 1)
    fore, aft = pl.ds(0, early_x.shape[1]), pl.ds(early_x.shape[1], late_x.shape[1])
    done += [local(dsend.at[1, low, fore], early_x), local(dsend.at[1, low, aft], late_x)]
    i_x.wait_recv()
    dh_part(2, 0, 0)
    done += [local(dsend.at[2, top, fore], early_y), local(dsend.at[2, top, aft], late_y)]
    for copy in g_cp:
        copy.wait_recv()
    h_cp = [remote(rb.at[zp[r]], ra.at[z], up[r]) for r in range(1, n)]
    ra[z] = rb[z]
    pl.loop(tiles, 2 * tiles)(g_tile)
    res_ld.wait()
    for copy in h_cp:
        copy.wait_recv()
    total = own_cot[...].astype(jnp.float32) + ra[...].reshape(rows, half).astype(jnp.float32)
    own_cot[...] = total.astype(jnp.bfloat16)
    done.append(local(own_cot, out_o))
    for i in (2 * tiles - 2, 2 * tiles - 1):
        for copy in g_copies(i):
            copy.wait()
    for copy in done:
        copy.wait()
    for copy in j_cp:
        copy.wait_recv()
    for copy in sends:
        if all(copy is not other for other in a_cp):
            copy.wait_send()


def write_kernel(out, g_text, g_image, out_o, gt_o, gi_o):
    out_o[...] = out[...]
    gt_o[...] = g_text[...]
    gi_o[...] = g_image[...]


def grad_kernel(own, got, last_x, last_y, gate, up, *refs):
    gg_o, gu_o = refs[-2:]
    height, count = own.shape[0], 16

    def rows_of(last):
        for i in range(height // count):
            at = pl.ds(i * count, count)
            d = own[at, :].astype(jnp.float32) + got[at, :].astype(jnp.float32) + last[at, :].astype(jnp.float32)
            gate_f, up_f, sig, act = silu_parts(gate[at, :], up[at, :])
            gg_o[at, :] = (d * up_f * sig * (1.0 + gate_f * (1.0 - sig))).astype(jnp.bfloat16)
            gu_o[at, :] = (d * act).astype(jnp.bfloat16)

    @pl.when(pl.program_id(0) == 0)
    def _():
        rows_of(last_y)

    @pl.when(pl.program_id(0) == 1)
    def _():
        rows_of(last_x)


def grad_call(own, got, last_x, last_y, gate, up, first, so_far):
    ff, rows = own.shape
    wide = min(last_x.shape[1], 4 * LANES)
    steps = last_x.shape[1] // wide
    tile = (ff // 2, wide)
    skip = first // wide
    every = pl.BlockSpec(tile, lambda a, j: (a, j + skip))
    anywhere = pl.BlockSpec(memory_space=pl.ANY)
    cells = 2 * last_x.shape[0] * last_x.shape[1]
    block = jax.ShapeDtypeStruct((ff, rows), jnp.bfloat16)
    return pl.pallas_call(
        grad_kernel,
        grid=(2, steps),
        out_shape=(block, block),
        in_specs=[
            every,
            every,
            pl.BlockSpec(tile, lambda a, j: (0, a * j)),
            pl.BlockSpec(tile, lambda a, j: (0, (1 - a) * j + a * (steps - 1))),
            every,
            every,
        ]
        + [anywhere] * len(so_far),
        out_specs=(every, every),
        input_output_aliases={6 + i: i for i in range(len(so_far))},
        compiler_params=pltpu.CompilerParams(
            dimension_semantics=("arbitrary", "arbitrary"), vmem_limit_bytes=VMEM_BYTES
        ),
        cost_estimate=pl.CostEstimate(flops=1000 * cells, bytes_accessed=14 * cells, transcendentals=cells),
        name="gate_grads",
    )(own, got, last_x, last_y, gate, up, *so_far)


def square_per_device(
    n_fsdp,
    n_tp,
    ref_gate,
    ref_up,
    ref_residual,
    ref_modality,
    ref_down_text,
    ref_down_image,
    pol_gate,
    pol_up,
    pol_modality,
    pol_segment,
    pair_margin,
    token_cotangent,
    pol_down_text,
    pol_down_image,
):
    rows, feats = token_cotangent.shape
    ff = ref_gate.shape[1]
    n = n_fsdp
    q = rows // n
    bf16 = jnp.bfloat16
    shape = jax.ShapeDtypeStruct
    block = shape((ff, rows), bf16)
    grad = shape((ff, 2 * feats), jnp.float32)
    anywhere = pl.BlockSpec(memory_space=pl.ANY)
    aft = rows // (3 * LANES) * LANES
    fore_part, aft_part = shape((ff // 2, rows - aft), bf16), shape((ff // 2, aft), bf16)
    outs = (
        shape((rows, feats), bf16), block, block, fore_part, aft_part, fore_part, aft_part, grad, grad,
    )
    scratch = [
        pltpu.VMEM((4, ff, rows), bf16),
        pltpu.VMEM((4, ff, rows), bf16),
        pltpu.VMEM((3, rows // LANES, LANES), jnp.int32),
        pltpu.VMEM((4, 16, rows), bf16),
        pltpu.VMEM((rows, feats), bf16),
        pltpu.VMEM((n, q, feats), bf16),
        pltpu.VMEM((2, 4, rows, feats), bf16),
        pltpu.VMEM((2, ff, 2 * feats), bf16),
        pltpu.VMEM((4, rows, feats), bf16),
        pltpu.VMEM((4, rows, feats), bf16),
        pltpu.VMEM((4, rows, feats), bf16),
        pltpu.VMEM((n - 1, 4, q, feats), bf16),
        pltpu.VMEM((4, q, feats), bf16),
        pltpu.VMEM((4, q, feats), bf16),
        pltpu.VMEM((4, q, feats), bf16),
        pltpu.VMEM((4, ff, rows), bf16),
        pltpu.VMEM((2, ff // 2, rows), bf16),
        pltpu.VMEM((2, 2, ff // 2, 2 * LANES), jnp.float32),
        pltpu.SemaphoreType.DMA((64,)),
        pltpu.SemaphoreType.DMA((64,)),
        pltpu.SemaphoreType.DMA((32,)),
        pltpu.SemaphoreType.DMA((2, 2)),
    ]
    out, own, got, early_x, late_x, early_y, late_y, g_text, g_image = pl.pallas_call(
        square_kernel,
        out_shape=outs,
        in_specs=[pl.BlockSpec(memory_space=pltpu.SMEM)] + [anywhere] * 13,
        out_specs=(anywhere,) * len(outs),
        scratch_shapes=scratch,
        compiler_params=pltpu.CompilerParams(
            collective_id=0, has_side_effects=True, vmem_limit_bytes=VMEM_BYTES
        ),
        name="square_step",
    )(
        pair_margin, ref_gate.T, ref_up.T, ref_residual, ref_modality.reshape(-1, LANES), ref_down_text.T, ref_down_image.T,
        pol_gate.T, pol_up.T, pol_modality.reshape(-1, LANES), pol_segment.reshape(-1, LANES), token_cotangent,
        pol_down_text.T, pol_down_image.T,
    )
    across_x = [(i, i + 1 - 2 * (i % 2)) for i in range(n)]
    across_y = [(i, (i + 2) % n) for i in range(n)]
    early_x = lax.ppermute(early_x, "fsdp", across_x)
    early_y = lax.ppermute(early_y, "fsdp", across_y)
    late_x = lax.ppermute(late_x, "fsdp", across_x)
    late_y = lax.ppermute(late_y, "fsdp", across_y)

    wide = 2 * LANES
    steps = 2 * feats // wide
    out_spec = pl.BlockSpec((rows // (2 * steps), feats), lambda a, j: (a * steps + j, 0))
    g_spec = pl.BlockSpec((ff // 2, wide), lambda a, j: (a, j))
    ref_out, g_text, g_image = pl.pallas_call(
        write_kernel,
        grid=(2, steps),
        out_shape=(shape((rows, feats), bf16), grad, grad),
        in_specs=[out_spec, g_spec, g_spec],
        out_specs=(out_spec, g_spec, g_spec),
        compiler_params=pltpu.CompilerParams(
            dimension_semantics=("arbitrary", "arbitrary"), vmem_limit_bytes=VMEM_BYTES
        ),
        cost_estimate=pl.CostEstimate(
            flops=1000 * ff * feats, bytes_accessed=32 * ff * feats, transcendentals=0
        ),
        name="write_out",
    )(out, g_text, g_image)

    grads = grad_call(own, got, early_x, early_y, pol_gate.T, pol_up.T, 0, ())
    grad_gate, grad_up = grad_call(own, got, late_x, late_y, pol_gate.T, pol_up.T, rows - aft, grads)
    return (ref_out, grad_gate.T, grad_up.T, g_text.T, g_image.T)


def solution(mesh):
    n_fsdp, n_tp = mesh.shape["fsdp"], mesh.shape["tp"]
    two = P("fsdp", "tp")
    one = P("fsdp")
    in_specs = (two, two, two, one, two, two, two, two, one, one, P(), two, two, two)
    square = n_fsdp == 4 and n_tp == 2 * n_fsdp
    plan = square_per_device if square else per_device

    def body(*args):
        return plan(n_fsdp, n_tp, *args)

    return jax.shard_map(
        body, mesh=mesh, in_specs=in_specs, out_specs=(two,) * 5, check_vma=False
    )
```
